32 devices in a mesh: dp: 2 (over x), ep: 16 (over z, y, core).
Axes of the slice: x: 2, y: 2, z: 4, core: 2. Of those that a mesh axis runs over, the one named last changes fastest.
Arguments:
- tok_rows: bfloat16 [16384, 2048], P(('dp', 'ep')), parts along dimension 0
- router_w: bfloat16 [2048, 64], replicated
- top_idx: int32 [16384, 6], P(('dp', 'ep')), parts along dimension 0
- slot_idx: int32 [16384, 6], P(('dp', 'ep')), parts along dimension 0
- w_gate: bfloat16 [80, 2048, 1408], P('ep')
- w_up: bfloat16 [80, 2048, 1408], P('ep')
- w_down: bfloat16 [80, 1408, 2048], P('ep')
- sh_gate: bfloat16 [2048, 2816], replicated
- sh_up: bfloat16 [2048, 2816], replicated
- sh_down: bfloat16 [2816, 2048], replicated
Outputs:
- output: bfloat16 [16384, 2048], P(('dp', 'ep')), parts along dimension 0
There are 2 independent parts. The reference program is written for one: setup_inputs(seed, part) draws one part's arguments, and reference() takes and returns one part's arrays. A program takes and returns all parts, laid end to end along the dimension named above; an argument that names none is the same for every part.
All inputs are finite; a program needn't handle non-finite values.
Results may differ from the reference program's by a relative error of at most 0.00103.
Values are sent between devices in bfloat16 or wider.
A program may use at most 1 GiB of HBM per device.

```python
import jax
import jax.numpy as jnp
from jax import lax

HIDDEN = 2048
EXPERT_FF = 1408
SHARED_FF = 2816
EXPERTS = 64
TOP_K = 6
GROUPS = 1
TOP_GROUPS = 1
TOK_DEV = 512
EP_DEVS = 16

PER_DEV = EXPERTS // EP_DEVS
DEV_SLOTS = PER_DEV + 1
NUM_SLOTS = EP_DEVS * DEV_SLOTS
TOKENS = EP_DEVS * TOK_DEV
GROUP_SIZE = EXPERTS // GROUPS
SLOT_CAP = ((2 * TOK_DEV * TOP_K + NUM_SLOTS - 1) // NUM_SLOTS + 7) // 8 * 8
SLOT_ROWS = EP_DEVS * SLOT_CAP
ROUTE_SCALE = 2.5
BIG_BONUS = 2 ** 20
RAND_TOP = 2 ** 16
FAR_BELOW = 2 ** 29


def draw_matrix(mat_key, fan_in, fan_out):
    return (jax.random.normal(mat_key, (fan_in, fan_out), jnp.float32) * fan_in ** -0.5).astype(jnp.bfloat16)


def expert_stack(stack_key, fan_in, fan_out):
    return lax.map(lambda one_key: draw_matrix(one_key, fan_in, fan_out), jax.random.split(stack_key, EXPERTS))


def slot_layout(order_key):
    popular = jax.random.permutation(order_key, EXPERTS).astype(jnp.int32)
    pop_rank = jnp.zeros((EXPERTS,), jnp.int32).at[popular].set(jnp.arange(EXPERTS, dtype=jnp.int32))
    slot_ids = jnp.arange(NUM_SLOTS, dtype=jnp.int32)
    slot_dev = slot_ids // DEV_SLOTS
    slot_local = slot_ids % DEV_SLOTS
    slot_expert = jnp.where(slot_local < PER_DEV, slot_dev * PER_DEV + slot_local, popular[slot_dev])
    return popular, pop_rank, slot_expert


def draw_routes(route_key, popular, pop_rank):
    expert_ids = jnp.arange(EXPERTS, dtype=jnp.int32)
    prim_slot = (expert_ids // PER_DEV) * DEV_SLOTS + expert_ids % PER_DEV
    has_spare = pop_rank < EP_DEVS
    spare_slot = jnp.where(has_spare, pop_rank * DEV_SLOTS + PER_DEV, 0)
    exp_bias = (RAND_TOP * (EXPERTS - pop_rank)) // EXPERTS + jnp.where(pop_rank == 0, BIG_BONUS, 0)
    grp_bias = jnp.where(jnp.arange(GROUPS) == popular[0] // GROUP_SIZE, BIG_BONUS, 0)
    key_exp, key_grp, key_rep = jax.random.split(route_key, 3)
    exp_rand = jax.random.randint(key_exp, (TOK_DEV, EP_DEVS, EXPERTS), 0, RAND_TOP, dtype=jnp.int32)
    grp_rand = jax.random.randint(key_grp, (TOK_DEV, EP_DEVS, GROUPS), 0, RAND_TOP, dtype=jnp.int32)
    rep_rand = jax.random.randint(key_rep, (TOK_DEV, EP_DEVS, TOP_K), 0, 4, dtype=jnp.int32)

    def route_step(slot_count, step_draws):
        step_exp, step_grp, step_rep = step_draws
        prim_ok = slot_count[:, prim_slot] < SLOT_CAP
        spare_ok = has_spare[None, :] & (slot_count[:, spare_slot] < SLOT_CAP)
        usable = prim_ok | spare_ok
        grp_usable = jnp.sum(usable.reshape(EP_DEVS, GROUPS, GROUP_SIZE).astype(jnp.int32), axis=2) >= TOP_K
        grp_score = (step_grp + grp_bias) * GROUPS + jnp.arange(GROUPS) - jnp.where(grp_usable, 0, FAR_BELOW)
        top_grp = lax.top_k(grp_score, TOP_GROUPS)[1]
        grp_taken = jnp.any(top_grp[:, :, None] == jnp.arange(GROUPS)[None, None, :], axis=1)
        exp_taken = jnp.repeat(grp_taken, GROUP_SIZE, axis=1)
        exp_score = (step_exp + exp_bias) * EXPERTS + expert_ids - jnp.where(usable, 0, FAR_BELOW) - jnp.where(exp_taken, 0, 2 * FAR_BELOW)
        top_exp = lax.top_k(exp_score, TOP_K)[1]
        prim_pick = jnp.take_along_axis(prim_ok, top_exp, axis=1)
        spare_pick = jnp.take_along_axis(spare_ok, top_exp, axis=1)
        use_spare = spare_pick & (jnp.logical_not(prim_pick) | (step_rep == 0))
        chosen = jnp.where(use_spare, spare_slot[top_exp], prim_slot[top_exp])
        slot_count = slot_count + jnp.sum((chosen[:, :, None] == jnp.arange(NUM_SLOTS)[None, None, :]).astype(jnp.int32), axis=1)
        return slot_count, (top_exp, chosen)

    start_count = jnp.zeros((EP_DEVS, NUM_SLOTS), jnp.int32)
    all_exp, all_slot = lax.scan(route_step, start_count, (exp_rand, grp_rand, rep_rand))[1]
    top_idx = jnp.transpose(all_exp, (1, 0, 2)).reshape(TOKENS, TOP_K).astype(jnp.int32)
    slot_idx = jnp.transpose(all_slot, (1, 0, 2)).reshape(TOKENS, TOP_K).astype(jnp.int32)
    return top_idx, slot_idx


def setup_inputs(seed: int = 0, part: int = 0) -> dict:
    shared_keys = jax.random.split(jax.random.key(seed), 8)
    part_keys = jax.random.split(jax.random.fold_in(jax.random.key(seed + 1), part), 2)
    popular, pop_rank, slot_expert = slot_layout(shared_keys[0])
    top_idx, slot_idx = draw_routes(part_keys[0], popular, pop_rank)
    tok_rows = jax.random.normal(part_keys[1], (TOKENS, HIDDEN), jnp.float32).astype(jnp.bfloat16)
    return {
        'tok_rows': tok_rows,
        'router_w': draw_matrix(shared_keys[1], HIDDEN, EXPERTS),
        'top_idx': top_idx,
        'slot_idx': slot_idx,
        'w_gate': jnp.take(expert_stack(shared_keys[2], HIDDEN, EXPERT_FF), slot_expert, axis=0),
        'w_up': jnp.take(expert_stack(shared_keys[3], HIDDEN, EXPERT_FF), slot_expert, axis=0),
        'w_down': jnp.take(expert_stack(shared_keys[4], EXPERT_FF, HIDDEN), slot_expert, axis=0),
        'sh_gate': draw_matrix(shared_keys[5], HIDDEN, SHARED_FF),
        'sh_up': draw_matrix(shared_keys[6], HIDDEN, SHARED_FF),
        'sh_down': draw_matrix(shared_keys[7], SHARED_FF, HIDDEN),
    }


def reference(tok_rows, router_w, top_idx, slot_idx, w_gate, w_up, w_down, sh_gate, sh_up, sh_down):
    scores = jax.nn.sigmoid(jnp.dot(tok_rows, router_w, preferred_element_type=jnp.float32))
    picked = jnp.take_along_axis(scores, top_idx, axis=1)
    gate_wts = picked / jnp.sum(picked, axis=1, keepdims=True) * ROUTE_SCALE
    flat_slot = slot_idx.reshape(-1)
    slot_hot = (flat_slot[:, None] == jnp.arange(NUM_SLOTS)[None, :]).astype(jnp.int32)
    slot_rank = jnp.sum(jnp.cumsum(slot_hot, axis=0) * slot_hot, axis=1) - 1
    dest_row = flat_slot * SLOT_ROWS + slot_rank
    row_token = jnp.full((NUM_SLOTS * SLOT_ROWS,), TOKENS, jnp.int32).at[dest_row].set(jnp.arange(TOKENS * TOP_K, dtype=jnp.int32) // TOP_K)

    def one_slot(slot_args):
        rows_at, gate_mat, up_mat, down_mat = slot_args
        slot_rows = jnp.take(tok_rows, rows_at, axis=0, mode='fill', fill_value=0)
        gate_act = jnp.dot(slot_rows, gate_mat, preferred_element_type=jnp.float32)
        up_act = jnp.dot(slot_rows, up_mat, preferred_element_type=jnp.float32)
        hid_act = (jax.nn.silu(gate_act) * up_act).astype(jnp.bfloat16)
        return jnp.dot(hid_act, down_mat, preferred_element_type=jnp.float32).astype(jnp.bfloat16)

    slot_out = lax.map(one_slot, (row_token.reshape(NUM_SLOTS, SLOT_ROWS), w_gate, w_up, w_down))
    per_choice = jnp.take(slot_out.reshape(NUM_SLOTS * SLOT_ROWS, HIDDEN), dest_row, axis=0).reshape(TOKENS, TOP_K, HIDDEN)
    routed = jnp.sum(per_choice.astype(jnp.float32) * gate_wts[:, :, None], axis=1)
    sh_hid = (jax.nn.silu(jnp.dot(tok_rows, sh_gate, preferred_element_type=jnp.float32)) * jnp.dot(tok_rows, sh_up, preferred_element_type=jnp.float32)).astype(jnp.bfloat16)
    shared_out = jnp.dot(sh_hid, sh_down, preferred_element_type=jnp.float32)
    return (shared_out + routed).astype(jnp.bfloat16)
```

```python
import jax
import jax.numpy as jnp
from jax import lax
from jax.sharding import PartitionSpec as P

ROUTE_SCALE = 2.5


def solution(mesh):
    ep_size = mesh.shape['ep']

    def local_block(tok_rows, router_w, top_idx, slot_idx, w_gate, w_up, w_down, sh_gate, sh_up, sh_down):
        tok_count, hidden = tok_rows.shape
        top_k = top_idx.shape[1]
        dev_slots = w_gate.shape[0]
        num_slots = ep_size * dev_slots
        slot_cap = ((2 * tok_count * top_k + num_slots - 1) // num_slots + 7) // 8 * 8
        pair_rows = dev_slots * slot_cap
        me = lax.axis_index('ep')
        logits = jnp.dot(tok_rows, router_w, preferred_element_type=jnp.float32)
        scores = jax.nn.sigmoid(logits)
        exp_ids = jnp.arange(router_w.shape[1], dtype=jnp.int32)
        picked = jnp.sum(jnp.where(top_idx[:, :, None] == exp_ids, scores[:, None, :], 0.0), axis=2)
        gate_wts = picked / jnp.sum(picked, axis=1, keepdims=True) * ROUTE_SCALE
        meta = jnp.concatenate([slot_idx.astype(jnp.float32), gate_wts], axis=1)
        all_meta = lax.all_gather(meta, 'ep', axis=0, tiled=True)
        all_rows = lax.all_gather(tok_rows, 'ep', axis=0, tiled=False)

        sh_hid = (jax.nn.silu(jnp.dot(tok_rows, sh_gate, preferred_element_type=jnp.float32)) * jnp.dot(tok_rows, sh_up, preferred_element_type=jnp.float32)).astype(jnp.bfloat16)
        shared_out = jnp.dot(sh_hid, sh_down, preferred_element_type=jnp.float32)

        all_slot = all_meta[:, :top_k].astype(jnp.int32) - me * dev_slots
        all_gate = all_meta[:, top_k:]
        local_ids = jnp.arange(dev_slots, dtype=jnp.int32)
        match = all_slot[:, :, None] == local_ids
        hot = jnp.any(match, axis=1).reshape(ep_size, tok_count, dev_slots)
        gate_of = jnp.sum(jnp.where(match, all_gate[:, :, None], 0.0), axis=1).reshape(ep_size, tok_count, dev_slots)
        before = (jnp.arange(tok_count)[:, None] > jnp.arange(tok_count)[None, :]).astype(jnp.bfloat16)
        rank = jnp.einsum('mn,pns->pms', before, hot.astype(jnp.bfloat16), preferred_element_type=jnp.float32).astype(jnp.int32)
        row_of = jnp.where(hot, rank + local_ids * slot_cap, -1)
        row_ids = jnp.arange(pair_rows, dtype=jnp.int32)
        pick = sum((row_of[:, None, :, s] == row_ids[None, :, None]).astype(jnp.bfloat16) for s in range(dev_slots))
        slot_rows = jnp.einsum('pkn,pnm->pkm', pick, all_rows, preferred_element_type=jnp.float32).astype(jnp.bfloat16)
        recv_rows = slot_rows.reshape(ep_size, dev_slots, slot_cap, hidden)
        gate_act = jnp.einsum('pskm,smf->spkf', recv_rows, w_gate, preferred_element_type=jnp.float32)
        up_act = jnp.einsum('pskm,smf->spkf', recv_rows, w_up, preferred_element_type=jnp.float32)
        hid_act = (jax.nn.silu(gate_act) * up_act).astype(jnp.bfloat16)
        exp_out = jnp.einsum('spkf,sfm->pskm', hid_act, w_down, preferred_element_type=jnp.float32).astype(jnp.bfloat16)
        exp_out = exp_out.reshape(ep_size, pair_rows, hidden)
        weigh = sum(jnp.where(row_of[:, :, s, None] == row_ids, gate_of[:, :, s, None], 0.0) for s in range(dev_slots))
        hi = lax.reduce_precision(weigh, 8, 7)
        mid = lax.reduce_precision(weigh - hi, 8, 7)
        low = weigh - hi - mid
        partial = sum(jnp.einsum('pnk,pkm->pnm', part.astype(jnp.bfloat16), exp_out, preferred_element_type=jnp.float32) for part in (low, mid, hi))
        routed = lax.psum_scatter(partial.reshape(ep_size * tok_count, hidden), 'ep', scatter_dimension=0, tiled=True)
        return (shared_out + routed).astype(jnp.bfloat16)

    tok_spec = P(('dp', 'ep'), None)
    slot_spec = P('ep', None, None)
    return jax.shard_map(local_block, mesh=mesh,
                         in_specs=(tok_spec, P(None, None), tok_spec, tok_spec, slot_spec, slot_spec, slot_spec,
                                   P(None, None), P(None, None), P(None, None)),
                         out_specs=tok_spec, check_vma=False)
```

```python
import functools

import jax
import jax.numpy as jnp
from jax import lax
from jax.experimental import pallas as pl
from jax.experimental.pallas import tpu as pltpu
from jax.sharding import PartitionSpec as P

ROUTE_SCALE = 2.5
MESH = pl.DeviceIdType.MESH


def ring_of(idx):
    z, y, core = idx // 4, (idx // 2) % 2, idx % 2
    return (z + y * (7 - 2 * z)) * 2 + core


def index_of(pos):
    pos = (pos + 32) % 16
    chip, core = pos // 2, pos % 2
    back = chip // 4
    z = chip + back * (7 - 2 * chip)
    return z * 4 + back * 2 + core


def reduce_kernel(hid_hbm, weigh_hbm, down_hbm, out_hbm, down_v, hid_v, weigh_v, tri_v, own_v, run_v,
                  down_sem, hid_sem, weigh_sem, send_sem, recv_sem, free_sem, out_sem):
    steps = weigh_hbm.shape[0]
    dev_slots, slot_cap, _ = hid_v.shape[2:]
    pair_rows = dev_slots * slot_cap
    half = run_v.shape[4]
    sub_rows = run_v.shape[3]
    col_tile = min(512, half)
    mix_tile = min(256, half)
    pos = ring_of(lax.axis_index('ep'))
    ahead = (index_of(pos + 1), index_of(pos - 1))
    behind = (index_of(pos - 1), index_of(pos + 1))

    barrier = pltpu.get_barrier_semaphore()
    for peer in ahead:
        pl.semaphore_signal(barrier, inc=1, device_id={'ep': peer}, device_id_type=MESH)

    def block_of(step, way):
        return index_of(pos - 1 - step) if way == 0 else index_of(pos + 1 + step)

    def fetches(step, way):
        par = step % 2
        block = block_of(step, way)
        return (pltpu.make_async_copy(hid_hbm.at[:, block], hid_v.at[par, way], hid_sem.at[par, way]),
                pltpu.make_async_copy(weigh_hbm.at[block], weigh_v.at[par, way], weigh_sem.at[par, way]))

    def start_fetch(step):
        for way in (0, 1):
            for copy in fetches(step, way):
                copy.start()

    def compute_own(step):
        par = step % 2
        for way in (0, 1):
            for copy in fetches(step, way):
                copy.wait()

            def one_slot(slot, _):
                for col in range(0, half, col_tile):
                    rows = jnp.dot(hid_v[par, way, slot], down_v[slot, :, way * half + col:way * half + col + col_tile],
                                   preferred_element_type=jnp.float32).astype(jnp.bfloat16)
                    for part in range(3):
                        at = pl.multiple_of(slot * slot_cap + part * pair_rows, 16)
                        tri_v[pl.ds(at, slot_cap), col:col + col_tile] = rows
                return 0

            lax.fori_loop(0, dev_slots, one_slot, 0)

            def one_tile(tile, _):
                cols = pl.ds(pl.multiple_of(tile * mix_tile, mix_tile), mix_tile)
                own_v[way, :, cols] = jnp.dot(weigh_v[par, way], tri_v[:, cols], preferred_element_type=jnp.float32)
                return 0

            lax.fori_loop(0, half // mix_tile, one_tile, 0)

    def send(step, way, sub):
        now, later = step % 2, (step + 1) % 2
        return pltpu.make_async_remote_copy(
            src_ref=run_v.at[way, now, sub], dst_ref=run_v.at[way, later, sub],
            send_sem=send_sem.at[way, now, sub], recv_sem=recv_sem.at[way, later, sub],
            device_id={'ep': ahead[way]}, device_id_type=MESH)

    down_copy = pltpu.make_async_copy(down_hbm, down_v, down_sem)
    down_copy.start()
    start_fetch(0)
    start_fetch(1)
    down_copy.wait()
    compute_own(0)
    start_fetch(2)
    pl.semaphore_wait(barrier, 2)
    for sub in (0, 1):
        for way in (0, 1):
            run_v[way, 0, sub] = own_v[way, sub * sub_rows:(sub + 1) * sub_rows, :]
            send(0, way, sub).start()
    compute_own(1)
    start_fetch(3)

    def one_step(step, _):
        now = step % 2
        for sub in (0, 1):
            for way in (0, 1):
                send(step - 1, way, sub).wait_recv()
                send(step - 1, way, sub).wait_send()
                pl.semaphore_signal(free_sem.at[way, sub], inc=1, device_id={'ep': behind[way]}, device_id_type=MESH)
                run_v[way, now, sub] += own_v[way, sub * sub_rows:(sub + 1) * sub_rows, :]
                pl.semaphore_wait(free_sem.at[way, sub], 1)
                send(step, way, sub).start()
        compute_own(step + 1)

        @pl.when(step + 3 < steps)
        def _():
            start_fetch(step + 3)
        return 0

    lax.fori_loop(1, steps - 1, one_step, 0)
    last = (steps - 1) % 2
    outs = []
    for sub in (0, 1):
        for way in (0, 1):
            send(steps - 2, way, sub).wait_recv()
            send(steps - 2, way, sub).wait_send()
            run_v[way, last, sub] += own_v[way, sub * sub_rows:(sub + 1) * sub_rows, :]
            outs.append(pltpu.make_async_copy(run_v.at[way, last, sub],
                                              out_hbm.at[pl.ds(sub * sub_rows, sub_rows), pl.ds(way * half, half)],
                                              out_sem.at[way, sub]))
            outs[-1].start()
    for copy in outs:
        copy.wait()


def reduce_home(hid, weigh, w_down):
    dev_slots, steps, slot_cap, ff = hid.shape
    tok_count = weigh.shape[1]
    hidden = w_down.shape[2]
    half, sub_rows = hidden // 2, tok_count // 2
    any_spec = pl.BlockSpec(memory_space=pl.ANY)
    dma = pltpu.SemaphoreType.DMA
    flops = 2 * steps * dev_slots * slot_cap * hidden * (ff + 3 * tok_count)
    return pl.pallas_call(
        reduce_kernel,
        out_shape=jax.ShapeDtypeStruct((tok_count, hidden), jnp.float32),
        in_specs=[any_spec] * 3,
        out_specs=any_spec,
        scratch_shapes=[
            pltpu.VMEM((dev_slots, ff, hidden), jnp.bfloat16),
            pltpu.VMEM((2, 2, dev_slots, slot_cap, ff), jnp.bfloat16),
            pltpu.VMEM((2, 2, tok_count, weigh.shape[2]), jnp.bfloat16),
            pltpu.VMEM((weigh.shape[2], half), jnp.bfloat16),
            pltpu.VMEM((2, tok_count, half), jnp.float32),
            pltpu.VMEM((2, 2, 2, sub_rows, half), jnp.float32),
            dma, dma((2, 2)), dma((2, 2)), dma((2, 2, 2)), dma((2, 2, 2)),
            pltpu.SemaphoreType.REGULAR((2, 2)), dma((2, 2)),
        ],
        compiler_params=pltpu.CompilerParams(collective_id=1, has_side_effects=True, vmem_limit_bytes=65_000_000),
        cost_estimate=pl.CostEstimate(flops=flops, bytes_accessed=70_000_000, transcendentals=0),
        name='reduce_home',
    )(hid, weigh, w_down)


def solution(mesh):
    ep_size = mesh.shape['ep']

    def local_block(tok_rows, router_w, top_idx, slot_idx, w_gate, w_up, w_down, sh_gate, sh_up, sh_down):
        tok_count, hidden = tok_rows.shape
        top_k = top_idx.shape[1]
        dev_slots = w_gate.shape[0]
        num_slots = ep_size * dev_slots
        slot_cap = ((2 * tok_count * top_k + num_slots - 1) // num_slots + 15) // 16 * 16
        pair_rows = dev_slots * slot_cap
        me = lax.axis_index('ep')
        logits = jnp.dot(tok_rows, router_w, preferred_element_type=jnp.float32)
        scores = jax.nn.sigmoid(logits)
        exp_ids = jnp.arange(router_w.shape[1], dtype=jnp.int32)
        picked = jnp.sum(jnp.where(top_idx[:, :, None] == exp_ids, scores[:, None, :], 0.0), axis=2)
        gate_wts = picked / jnp.sum(picked, axis=1, keepdims=True) * ROUTE_SCALE
        meta = jnp.concatenate([slot_idx.astype(jnp.float32), gate_wts], axis=1)
        all_meta = lax.all_gather(meta, 'ep', axis=0, tiled=True)
        all_rows = lax.all_gather(tok_rows, 'ep', axis=0, tiled=False)

        sh_hid = (jax.nn.silu(jnp.dot(tok_rows, sh_gate, preferred_element_type=jnp.float32)) * jnp.dot(tok_rows, sh_up, preferred_element_type=jnp.float32)).astype(jnp.bfloat16)
        shared_out = jnp.dot(sh_hid, sh_down, preferred_element_type=jnp.float32)

        all_slot = all_meta[:, :top_k].astype(jnp.int32) - me * dev_slots
        all_gate = all_meta[:, top_k:]
        local_ids = jnp.arange(dev_slots, dtype=jnp.int32)
        match = all_slot[:, :, None] == local_ids
        hot = jnp.any(match, axis=1).reshape(ep_size, tok_count, dev_slots)
        gate_of = jnp.sum(jnp.where(match, all_gate[:, :, None], 0.0), axis=1).reshape(ep_size, tok_count, dev_slots)
        before = (jnp.arange(tok_count)[:, None] > jnp.arange(tok_count)[None, :]).astype(jnp.bfloat16)
        rank = jnp.einsum('mn,pns->pms', before, hot.astype(jnp.bfloat16), preferred_element_type=jnp.float32).astype(jnp.int32)
        row_of = jnp.where(hot, rank + local_ids * slot_cap, -1)
        row_ids = jnp.arange(pair_rows, dtype=jnp.int32)
        weigh = sum(jnp.where(row_of[:, :, s, None] == row_ids, gate_of[:, :, s, None], 0.0) for s in range(dev_slots))
        hi = lax.reduce_precision(weigh, 8, 7)
        mid = lax.reduce_precision(weigh - hi, 8, 7)
        low = weigh - hi - mid
        weigh3 = jnp.concatenate([low.astype(jnp.bfloat16), mid.astype(jnp.bfloat16), hi.astype(jnp.bfloat16)], axis=2)
        pick = sum((row_of[:, None, :, s] == row_ids[None, :, None]).astype(jnp.bfloat16) for s in range(dev_slots))
        slot_rows = jnp.einsum('pkn,pnm->pkm', pick, all_rows, preferred_element_type=jnp.float32).astype(jnp.bfloat16)
        recv_rows = slot_rows.reshape(ep_size, dev_slots, slot_cap, hidden)
        gate_act = jnp.einsum('pskm,smf->spkf', recv_rows, w_gate, preferred_element_type=jnp.float32)
        up_act = jnp.einsum('pskm,smf->spkf', recv_rows, w_up, preferred_element_type=jnp.float32)
        hid_act = (jax.nn.silu(gate_act) * up_act).astype(jnp.bfloat16)
        routed = reduce_home(hid_act, weigh3, w_down)
        return (shared_out + routed).astype(jnp.bfloat16)

    tok_spec = P(('dp', 'ep'), None)
    slot_spec = P('ep', None, None)
    return jax.shard_map(local_block, mesh=mesh,
                         in_specs=(tok_spec, P(None, None), tok_spec, tok_spec, slot_spec, slot_spec, slot_spec,
                                   P(None, None), P(None, None), P(None, None)),
                         out_specs=tok_spec, check_vma=False)
```

```python
import functools

import jax
import jax.numpy as jnp
from jax import lax
from jax.experimental import pallas as pl
from jax.experimental.pallas import tpu as pltpu
from jax.sharding import PartitionSpec as P

ROUTE_SCALE = 2.5
MESH = pl.DeviceIdType.MESH


def ring_of(idx):
    z, y, core = idx // 4, (idx // 2) % 2, idx % 2
    return (z + y * (7 - 2 * z)) * 2 + core


def index_of(pos):
    pos = (pos + 32) % 16
    chip, core = pos // 2, pos % 2
    back = chip // 4
    z = chip + back * (7 - 2 * chip)
    return z * 4 + back * 2 + core


def gather_kernel(tok_hbm, meta_hbm, gate_hbm, up_hbm, shg_hbm, shu_hbm, shd_hbm, hid_hbm, all_meta_hbm, z_hbm,
                  tok_v, meta_v, rows_v, w_v, h_v, z_v,
                  tok_sem, own_sem, w_sem, h_sem, z_sem, keep_sem, send_sem, recv_sem, msend_sem, mrecv_sem):
    ring, _, sub_rows, hidden = tok_v.shape
    dev_slots = rows_v.shape[0]
    ff = h_v.shape[2]
    tok_count = 2 * sub_rows
    slot_cap = hid_hbm.shape[2]
    pair_rows = dev_slots * slot_cap
    bufs = w_v.shape[0]
    tiles = ff // 128
    far = ring // 2
    chunks = ring - 1
    me = lax.axis_index('ep')
    pos = ring_of(me)
    ahead = (index_of(pos + 1), index_of(pos - 1))
    col_tile = min(512, hidden)

    barrier = pltpu.get_barrier_semaphore()
    for off in range(1, ring):
        pl.semaphore_signal(barrier, inc=1, device_id={'ep': index_of(pos + off)}, device_id_type=MESH)

    own_meta = pltpu.make_async_copy(meta_hbm, meta_v.at[0], own_sem.at[0])
    own_toks = [pltpu.make_async_copy(tok_hbm.at[pl.ds(sub * sub_rows, sub_rows)], tok_v.at[0, sub], tok_sem.at[sub]) for sub in (0, 1)]
    own_meta.start()
    for copy in own_toks:
        copy.start()

    def chunk(i, way):
        dist = (i + 1) // 2
        sub = way if isinstance(i, int) and i == chunks else (i + 1) % 2
        if way == 0:
            src, dst = (ring + 1 - dist) % ring, ring - dist
        else:
            src, dst = dist - 1, dist
        return pltpu.make_async_remote_copy(
            src_ref=tok_v.at[src, sub], dst_ref=tok_v.at[dst, sub],
            send_sem=send_sem.at[way, i - 1], recv_sem=recv_sem.at[way, i - 1],
            device_id={'ep': ahead[way]}, device_id_type=MESH)

    def tick(i):
        for way in (0, 1):
            chunk(i, way).wait_recv()
            chunk(i + 2, way).start()

    def meta_copy(off):
        return pltpu.make_async_remote_copy(
            src_ref=meta_v.at[0], dst_ref=meta_v.at[ring - off],
            send_sem=msend_sem.at[off - 1], recv_sem=mrecv_sem.at[ring - off - 1],
            device_id={'ep': index_of(pos + off)}, device_id_type=MESH)

    def stream(copies_of, use, low, high, total):
        def body(i, _):
            for copy in copies_of(i):
                copy.wait()
            use(i, i % bufs)

            @pl.when(i + bufs < total)
            def _():
                for copy in copies_of(i + bufs):
                    copy.start()
            return 0
        lax.fori_loop(low, high, body, 0)

    def open_stream(copies_of):
        for i in range(bufs):
            for copy in copies_of(i):
                copy.start()

    def shared_copies(i):
        cols = pl.ds(pl.multiple_of(i * 128, 128), 128)
        return (pltpu.make_async_copy(shg_hbm.at[:, cols], w_v.at[i % bufs, :, pl.ds(0, 128)], w_sem.at[i % bufs, 0]),
                pltpu.make_async_copy(shu_hbm.at[:, cols], w_v.at[i % bufs, :, pl.ds(128, 128)], w_sem.at[i % bufs, 1]))

    def shared_use(i, buf):
        cols = pl.ds(pl.multiple_of(i % tiles * 128, 128), 128)
        for sub in (0, 1):
            both = jnp.dot(tok_v[0, sub], w_v[buf], preferred_element_type=jnp.float32)
            h_v[i // tiles, sub * sub_rows:(sub + 1) * sub_rows, cols] = (jax.nn.silu(both[:, :128]) * both[:, 128:]).astype(jnp.bfloat16)

    def last_copies(i):
        cols = pl.ds(pl.multiple_of(i // 2 * 256, 256), 256)
        rows = pl.ds(pl.multiple_of(i % 2 * ff, 128), ff)
        return (pltpu.make_async_copy(shd_hbm.at[rows, cols], w_v.at[i % bufs, pl.ds(0, ff), :], w_sem.at[i % bufs, 0]),)

    def z_copy(tile):
        cols = pl.ds(pl.multiple_of(tile * 256, 256), 256)
        return pltpu.make_async_copy(z_v.at[tile % 2], z_hbm.at[:, cols], z_sem.at[tile % 2])

    def last_use(i, buf):
        tile = i // 2
        part = jnp.dot(h_v[i % 2, :tok_count, :], w_v[buf, :ff, :], preferred_element_type=jnp.float32)

        @pl.when(i % 2 == 0)
        def _():
            @pl.when(tile >= 2)
            def _():
                z_copy(tile - 2).wait()
            z_v[tile % 2] = part

        @pl.when(i % 2 == 1)
        def _():
            z_v[tile % 2] += part
            z_copy(tile).start()

    def slot_copies(i):
        slot, tile = i // tiles, i % tiles
        cols = pl.ds(pl.multiple_of(tile * 128, 128), 128)
        return (pltpu.make_async_copy(gate_hbm.at[slot, :, cols], w_v.at[i % bufs, :, pl.ds(0, 128)], w_sem.at[i % bufs, 0]),
                pltpu.make_async_copy(up_hbm.at[slot, :, cols], w_v.at[i % bufs, :, pl.ds(128, 128)], w_sem.at[i % bufs, 1]))

    def slot_use(count):
        def use(i, buf):
            slot, tile = i // tiles, i % tiles
            both = jnp.dot(rows_v[slot, :count * slot_cap, :], w_v[buf], preferred_element_type=jnp.float32)
            cols = pl.ds(pl.multiple_of(tile * 128, 128), 128)
            h_v[slot % 2, :count * slot_cap, cols] = (jax.nn.silu(both[:, :128]) * both[:, 128:]).astype(jnp.bfloat16)
        return use

    def dispatch(block, place):
        ids = (lax.broadcasted_iota(jnp.int32, (pair_rows, 1), 0) + me * pair_rows).astype(jnp.float32)
        hit = meta_v[block, 0:1, :] == ids
        for j in range(1, 6):
            hit = hit | (meta_v[block, j:j + 1, :] == ids)
        pick = hit.astype(jnp.float32).astype(jnp.bfloat16)

        def one_tile(tile, _):
            cols = pl.ds(pl.multiple_of(tile * col_tile, col_tile), col_tile)
            rows = jnp.dot(pick[:, :sub_rows], tok_v[block, 0, :, cols], preferred_element_type=jnp.float32)
            rows += jnp.dot(pick[:, sub_rows:], tok_v[block, 1, :, cols], preferred_element_type=jnp.float32)
            rows = rows.astype(jnp.bfloat16)
            at = pl.multiple_of(place * slot_cap, 16)
            for slot in range(dev_slots):
                rows_v[slot, pl.ds(at, slot_cap), cols] = rows[slot * slot_cap:(slot + 1) * slot_cap]
            return 0
        lax.fori_loop(0, hidden // col_tile, one_tile, 0)

    near = [0] + [r for dist in range(1, far // 2 + 1) for r in (ring - dist, dist)]
    away = [r for dist in range(far // 2 + 1, far) for r in (ring - dist, dist)] + [far]

    def group(blocks, tick_from):
        def hid_copies(slot):
            return [pltpu.make_async_copy(h_v.at[slot % 2, pl.ds(k * slot_cap, slot_cap), :], hid_hbm.at[slot, r], h_sem.at[slot % 2, k])
                    for k, r in enumerate(blocks)]

        def one_slot(slot, _):
            @pl.when(slot >= 2)
            def _():
                for copy in hid_copies(slot - 2):
                    copy.wait()
            stream(slot_copies, slot_use(len(blocks)), slot * tiles, (slot + 1) * tiles, dev_slots * tiles)
            for copy in hid_copies(slot):
                copy.start()
            if tick_from is not None:
                @pl.when(slot < 4)
                def _():
                    tick(tick_from + slot)
            return 0
        lax.fori_loop(0, dev_slots, one_slot, 0)
        for slot in (dev_slots - 2, dev_slots - 1):
            for copy in hid_copies(slot):
                copy.wait()

    open_stream(shared_copies)
    own_meta.wait()
    for copy in own_toks:
        copy.wait()
    pl.semaphore_wait(barrier, ring - 1)
    for off in range(1, ring):
        meta_copy(off).start()
    for i in (1, 2):
        for way in (0, 1):
            chunk(i, way).start()
    stream(shared_copies, shared_use, 0, tiles, 2 * tiles)
    tick(1)
    stream(shared_copies, shared_use, tiles, 2 * tiles, 2 * tiles)
    open_stream(last_copies)
    for off in range(1, ring):
        meta_copy(off).wait_recv()
    keep = pltpu.make_async_copy(meta_v, all_meta_hbm, keep_sem)
    keep.start()
    tick(2)
    downs = 2 * (hidden // 256)
    stream(last_copies, last_use, 0, downs, downs)
    tick(3)
    open_stream(slot_copies)
    for tile in (hidden // 256 - 2, hidden // 256 - 1):
        z_copy(tile).wait()
    tick(4)
    dispatch(0, 0)

    def one_pair(dist, _):
        @pl.when(dist >= 3)
        def _():
            tick(2 * dist - 1)
            tick(2 * dist)
        dispatch(ring - dist, 2 * dist - 1)
        dispatch(dist, 2 * dist)
        return 0
    lax.fori_loop(1, far // 2 + 1, one_pair, 0)
    group(near, 2 * (far // 2) + 1)
    open_stream(slot_copies)

    def far_pair(dist, _):
        dispatch(ring - dist, 2 * dist - far - 2)
        dispatch(dist, 2 * dist - far - 1)
        return 0
    lax.fori_loop(far // 2 + 1, far - 1, far_pair, 0)
    chunk(chunks - 2, 0).wait_recv()
    chunk(chunks - 2, 1).wait_recv()
    chunk(chunks, 0).start()
    chunk(chunks - 1, 0).wait_recv()
    chunk(chunks - 1, 1).wait_recv()
    chunk(chunks, 1).start()
    far_pair(far - 1, 0)
    chunk(chunks, 0).wait_recv()
    chunk(chunks, 1).wait_recv()
    dispatch(far, far - 2)
    group(away, None)
    keep.wait()
    for off in range(1, ring):
        meta_copy(off).wait_send()
    for i in range(1, ring):
        for way in (0, 1):
            chunk(i, way).wait_send()


def gather_rows(tok_rows, meta, w_gate, w_up, sh_gate, sh_up, sh_down, ring, slot_cap):
    tok_count, hidden = tok_rows.shape
    dev_slots, _, ff = w_gate.shape
    any_spec = pl.BlockSpec(memory_space=pl.ANY)
    dma = pltpu.SemaphoreType.DMA
    near = ring // 2 + 1
    flops = 4 * hidden * ff * ring * dev_slots * slot_cap + 12 * tok_count * hidden * ff
    return pl.pallas_call(
        gather_kernel,
        out_shape=(jax.ShapeDtypeStruct((dev_slots, ring, slot_cap, ff), jnp.bfloat16),
                   jax.ShapeDtypeStruct((ring,) + meta.shape, jnp.float32),
                   jax.ShapeDtypeStruct((tok_count, hidden), jnp.float32)),
        in_specs=[any_spec] * 7,
        out_specs=(any_spec,) * 3,
        scratch_shapes=[
            pltpu.VMEM((ring, 2, tok_count // 2, hidden), jnp.bfloat16),
            pltpu.VMEM((ring,) + meta.shape, jnp.float32),
            pltpu.VMEM((dev_slots, near * slot_cap, hidden), jnp.bfloat16),
            pltpu.VMEM((4, hidden, 256), jnp.bfloat16),
            pltpu.VMEM((2, near * slot_cap, ff), jnp.bfloat16),
            pltpu.VMEM((2, tok_count, 256), jnp.float32),
            dma((2,)), dma((1,)), dma((4, 2)), dma((2, near)), dma((2,)), dma,
            dma((2, ring - 1)), dma((2, ring - 1)), dma((ring - 1,)), dma((ring - 1,)),
        ],
        compiler_params=pltpu.CompilerParams(collective_id=2, has_side_effects=True, vmem_limit_bytes=66_000_000),
        cost_estimate=pl.CostEstimate(flops=flops, bytes_accessed=170_000_000, transcendentals=0),
        name='gather_rows',
    )(tok_rows, meta, w_gate, w_up, sh_gate, sh_up, sh_down)


def reduce_kernel(hid_hbm, meta_hbm, down_hbm, out_hbm, down_v, hid_v, meta_v, weigh_v, tri_v, own_v, run_v,
                  down_sem, hid_sem, meta_sem, send_sem, recv_sem, free_sem, out_sem):
    steps = meta_hbm.shape[0]
    dev_slots, slot_cap, _ = hid_v.shape[2:]
    pair_rows = dev_slots * slot_cap
    half = run_v.shape[4]
    sub_rows = run_v.shape[3]
    col_tile = min(512, half)
    mix_tile = min(256, half)
    tok_tile = min(128, 2 * sub_rows)
    wide = weigh_v.shape[1] // 3
    me = lax.axis_index('ep')
    pos = ring_of(me)
    ahead = (index_of(pos + 1), index_of(pos - 1))
    behind = (index_of(pos - 1), index_of(pos + 1))

    barrier = pltpu.get_barrier_semaphore()
    for peer in ahead:
        pl.semaphore_signal(barrier, inc=1, device_id={'ep': peer}, device_id_type=MESH)

    def block_of(step, way):
        return steps - 1 - step if way == 0 else (step + 1) % steps

    def fetches(step, way):
        par = step % 2
        block = block_of(step, way)
        return (pltpu.make_async_copy(hid_hbm.at[:, block], hid_v.at[par, way], hid_sem.at[par, way]),
                pltpu.make_async_copy(meta_hbm.at[block], meta_v.at[par, way], meta_sem.at[par, way]))

    def start_fetch(step):
        for way in (0, 1):
            for copy in fetches(step, way):
                copy.start()

    def down_copy(slot):
        return pltpu.make_async_copy(down_hbm.at[slot], down_v.at[slot], down_sem.at[slot])

    def build_weigh(par, way):
        lane = lax.broadcasted_iota(jnp.int32, (1, wide), 1)
        ids = jnp.where(lane < pair_rows, lane + me * pair_rows, -1).astype(jnp.float32)

        def one_tile(tile, _):
            toks = pl.ds(pl.multiple_of(tile * tok_tile, tok_tile), tok_tile)
            info = jnp.transpose(meta_v[par, way, :, toks])
            weigh = jnp.zeros((tok_tile, wide), jnp.float32)
            for j in range(6):
                weigh = jnp.where(info[:, j:j + 1] == ids, info[:, 6 + j:7 + j], weigh)
            hi = weigh.astype(jnp.bfloat16)
            rest = weigh - hi.astype(jnp.float32)
            mid = rest.astype(jnp.bfloat16)
            low = (rest - mid.astype(jnp.float32)).astype(jnp.bfloat16)
            weigh_v[toks, :wide] = low
            weigh_v[toks, wide:2 * wide] = mid
            weigh_v[toks, 2 * wide:] = hi
            return 0
        lax.fori_loop(0, 2 * sub_rows // tok_tile, one_tile, 0)

    def compute_own(step, first=False):
        par = step % 2
        for way in (0, 1):
            for copy in fetches(step, way):
                copy.wait()
            build_weigh(par, way)

            def one_slot(slot, _):
                if first and way == 0:
                    down_copy(slot).wait()
                for col in range(0, half, col_tile):
                    rows = jnp.dot(hid_v[par, way, slot], down_v[slot, :, way * half + col:way * half + col + col_tile],
                                   preferred_element_type=jnp.float32).astype(jnp.bfloat16)
                    for part in range(3):
                        at = pl.multiple_of(slot * slot_cap + part * wide, 16)
                        tri_v[pl.ds(at, slot_cap), col:col + col_tile] = rows
                return 0

            lax.fori_loop(0, dev_slots, one_slot, 0)

            def one_tile(tile, _):
                cols = pl.ds(pl.multiple_of(tile * mix_tile, mix_tile), mix_tile)
                own_v[way, :, cols] = jnp.dot(weigh_v[...], tri_v[:, cols], preferred_element_type=jnp.float32)
                return 0

            lax.fori_loop(0, half // mix_tile, one_tile, 0)

    def send(step, way, sub):
        now, later = step % 2, (step + 1) % 2
        return pltpu.make_async_remote_copy(
            src_ref=run_v.at[way, now, sub], dst_ref=run_v.at[way, later, sub],
            send_sem=send_sem.at[way, now, sub], recv_sem=recv_sem.at[way, later, sub],
            device_id={'ep': ahead[way]}, device_id_type=MESH)

    start_fetch(0)
    for slot in range(dev_slots):
        down_copy(slot).start()
    start_fetch(1)
    tri_v[...] = jnp.zeros_like(tri_v)
    compute_own(0, True)
    start_fetch(2)
    pl.semaphore_wait(barrier, 2)
    for sub in (0, 1):
        for way in (0, 1):
            run_v[way, 0, sub] = own_v[way, sub * sub_rows:(sub + 1) * sub_rows, :]
            send(0, way, sub).start()
    compute_own(1)
    start_fetch(3)

    def one_step(step, _):
        now = step % 2
        for sub in (0, 1):
            for way in (0, 1):
                send(step - 1, way, sub).wait_recv()
                send(step - 1, way, sub).wait_send()
                pl.semaphore_signal(free_sem.at[way, sub], inc=1, device_id={'ep': behind[way]}, device_id_type=MESH)
                run_v[way, now, sub] += own_v[way, sub * sub_rows:(sub + 1) * sub_rows, :]
                pl.semaphore_wait(free_sem.at[way, sub], 1)
                send(step, way, sub).start()
        compute_own(step + 1)

        @pl.when(step + 3 < steps)
        def _():
            start_fetch(step + 3)
        return 0

    lax.fori_loop(1, steps - 1, one_step, 0)
    last = (steps - 1) % 2
    outs = []
    for sub in (0, 1):
        for way in (0, 1):
            send(steps - 2, way, sub).wait_recv()
            send(steps - 2, way, sub).wait_send()
            run_v[way, last, sub] += own_v[way, sub * sub_rows:(sub + 1) * sub_rows, :]
            outs.append(pltpu.make_async_copy(run_v.at[way, last, sub],
                                              out_hbm.at[pl.ds(sub * sub_rows, sub_rows), pl.ds(way * half, half)],
                                              out_sem.at[way, sub]))
            outs[-1].start()
    for copy in outs:
        copy.wait()


def reduce_home(hid, meta, w_down):
    dev_slots, steps, slot_cap, ff = hid.shape
    tok_count = meta.shape[2]
    wide = (dev_slots * slot_cap + 127) // 128 * 128
    hidden = w_down.shape[2]
    half, sub_rows = hidden // 2, tok_count // 2
    any_spec = pl.BlockSpec(memory_space=pl.ANY)
    dma = pltpu.SemaphoreType.DMA
    flops = 2 * steps * dev_slots * slot_cap * hidden * (ff + 3 * tok_count)
    return pl.pallas_call(
        reduce_kernel,
        out_shape=jax.ShapeDtypeStruct((tok_count, hidden), jnp.float32),
        in_specs=[any_spec] * 3,
        out_specs=any_spec,
        scratch_shapes=[
            pltpu.VMEM((dev_slots, ff, hidden), jnp.bfloat16),
            pltpu.VMEM((2, 2, dev_slots, slot_cap, ff), jnp.bfloat16),
            pltpu.VMEM((2, 2) + meta.shape[1:], jnp.float32),
            pltpu.VMEM((tok_count, 3 * wide), jnp.bfloat16),
            pltpu.VMEM((3 * wide, half), jnp.bfloat16),
            pltpu.VMEM((2, tok_count, half), jnp.float32),
            pltpu.VMEM((2, 2, 2, sub_rows, half), jnp.float32),
            dma((dev_slots,)), dma((2, 2)), dma((2, 2)), dma((2, 2, 2)), dma((2, 2, 2)),
            pltpu.SemaphoreType.REGULAR((2, 2)), dma((2, 2)),
        ],
        compiler_params=pltpu.CompilerParams(collective_id=1, has_side_effects=True, vmem_limit_bytes=65_000_000),
        cost_estimate=pl.CostEstimate(flops=flops, bytes_accessed=70_000_000, transcendentals=0),
        name='reduce_home',
    )(hid, meta, w_down)


def solution(mesh):
    ep_size = mesh.shape['ep']

    def local_block(tok_rows, router_w, top_idx, slot_idx, w_gate, w_up, w_down, sh_gate, sh_up, sh_down):
        tok_count = tok_rows.shape[0]
        top_k = top_idx.shape[1]
        dev_slots = w_gate.shape[0]
        num_slots = ep_size * dev_slots
        slot_cap = ((2 * tok_count * top_k + num_slots - 1) // num_slots + 15) // 16 * 16
        logits = jnp.dot(tok_rows, router_w, preferred_element_type=jnp.float32)
        scores = jax.nn.sigmoid(logits)
        exp_ids = jnp.arange(router_w.shape[1], dtype=jnp.int32)
        picked = jnp.sum(jnp.where(top_idx[:, :, None] == exp_ids, scores[:, None, :], 0.0), axis=2)
        gate_wts = picked / jnp.sum(picked, axis=1, keepdims=True) * ROUTE_SCALE
        match = slot_idx[:, :, None] == jnp.arange(num_slots, dtype=jnp.int32)
        hot = jnp.any(match, axis=1)
        before = (jnp.arange(tok_count)[:, None] > jnp.arange(tok_count)[None, :]).astype(jnp.bfloat16)
        rank = jnp.dot(before, hot.astype(jnp.bfloat16), preferred_element_type=jnp.float32)
        dest = slot_idx.astype(jnp.float32) * slot_cap + jnp.sum(jnp.where(match, rank[:, None, :], 0.0), axis=2)
        meta = jnp.concatenate([dest, gate_wts, jnp.zeros((tok_count, 16 - 2 * top_k), jnp.float32)], axis=1).T
        hid, all_meta, shared_out = gather_rows(tok_rows, meta, w_gate, w_up, sh_gate, sh_up, sh_down, ep_size, slot_cap)
        routed = reduce_home(hid, all_meta, w_down)
        return (shared_out + routed).astype(jnp.bfloat16)

    tok_spec = P(('dp', 'ep'), None)
    slot_spec = P('ep', None, None)
    return jax.shard_map(local_block, mesh=mesh,
                         in_specs=(tok_spec, P(None, None), tok_spec, tok_spec, slot_spec, slot_spec, slot_spec,
                                   P(None, None), P(None, None), P(None, None)),
                         out_specs=tok_spec, check_vma=False)
```

```python
import functools

import jax
import jax.numpy as jnp
from jax import lax
from jax.experimental import pallas as pl
from jax.experimental.pallas import tpu as pltpu
from jax.sharding import PartitionSpec as P

ROUTE_SCALE = 2.5
MESH = pl.DeviceIdType.MESH


def ring_of(idx):
    z, y, core = idx // 4, (idx // 2) % 2, idx % 2
    return (z + y * (7 - 2 * z)) * 2 + core


def index_of(pos):
    pos = (pos + 32) % 16
    chip, core = pos // 2, pos % 2
    back = chip // 4
    z = chip + back * (7 - 2 * chip)
    return z * 4 + back * 2 + core


SEG = 12


def slot_stream(gate_hbm, up_hbm, down_hbm, rows_v, w_v, h_v, y_v, y_hbm, w_sem, y_sem):
    dev_slots, rows = rows_v.shape[:2]
    ff = h_v.shape[1]
    bufs = w_v.shape[0]
    ups, downs = ff // 128, rows_v.shape[2] // 256
    per_slot = ups + downs
    total = dev_slots * per_slot
    slot_cap = y_v.shape[2]

    def up_copies(i):
        slot, tile = i // per_slot, i % per_slot
        cols = pl.ds(pl.multiple_of(tile * 128, 128), 128)
        return (pltpu.make_async_copy(gate_hbm.at[slot, :, cols], w_v.at[i % bufs, :, pl.ds(0, 128)], w_sem.at[i % bufs, 0]),
                pltpu.make_async_copy(up_hbm.at[slot, :, cols], w_v.at[i % bufs, :, pl.ds(128, 128)], w_sem.at[i % bufs, 1]))

    def down_copies(i):
        slot, tile = i // per_slot, i % per_slot - ups
        cols = pl.ds(pl.multiple_of(tile * 256, 256), 256)
        return (pltpu.make_async_copy(down_hbm.at[slot, :, cols], w_v.at[i % bufs, pl.ds(0, ff), :], w_sem.at[i % bufs, 0]),)

    def fetch(i):
        @pl.when(i % per_slot < ups)
        def _():
            for copy in up_copies(i):
                copy.start()

        @pl.when(i % per_slot >= ups)
        def _():
            for copy in down_copies(i):
                copy.start()

    def y_copy(slot, tile):
        cols = pl.ds(pl.multiple_of(tile * 256, 256), 256)
        at = pl.ds(pl.multiple_of(slot * slot_cap, 16), slot_cap)
        return pltpu.make_async_copy(y_v.at[tile % 2], y_hbm.at[:, at, cols], y_sem.at[tile % 2])

    def one(i, _):
        slot, k, buf = i // per_slot, i % per_slot, i % bufs

        @pl.when(k < ups)
        def _():
            for copy in up_copies(i):
                copy.wait()
            both = jnp.dot(rows_v[slot], w_v[buf], preferred_element_type=jnp.float32)
            cols = pl.ds(pl.multiple_of(k * 128, 128), 128)
            h_v[:rows, cols] = (jax.nn.silu(both[:, :128]) * both[:, 128:]).astype(jnp.bfloat16)

        @pl.when(k >= ups)
        def _():
            for copy in down_copies(i):
                copy.wait()
            tile = k - ups

            @pl.when((slot > 0) | (tile >= 2))
            def _():
                y_copy(slot, tile).wait()
            outs = jnp.dot(h_v[:rows, :], w_v[buf, :ff, :], preferred_element_type=jnp.float32).astype(jnp.bfloat16)
            y_v[tile % 2] = outs.reshape(rows // slot_cap, slot_cap, 256)
            y_copy(slot, tile).start()

        @pl.when(i + bufs < total)
        def _():
            fetch(i + bufs)
        return 0

    def open_all():
        for i in range(bufs):
            fetch(jnp.int32(i))

    def run(seg):
        lax.fori_loop(seg * SEG, jnp.minimum(seg * SEG + SEG, total), one, 0)

    def close():
        for tile in (downs - 2, downs - 1):
            y_copy(dev_slots - 1, tile).wait()

    return open_all, run, close, -(-total // SEG)


def gather_kernel(tok_hbm, meta_hbm, gate_hbm, up_hbm, down_hbm, shg_hbm, shu_hbm, shd_hbm, y_hbm, far_hbm, all_meta_hbm, z_hbm,
                  tok_v, meta_v, rows_v, far_v, w_v, h_v, y_v, z_v,
                  tok_sem, own_sem, w_sem, y_sem, far_sem, z_sem, keep_sem, send_sem, recv_sem, msend_sem, mrecv_sem):
    ring, _, sub_rows, hidden = tok_v.shape
    dev_slots = rows_v.shape[0]
    ff = h_v.shape[2]
    tok_count = 2 * sub_rows
    slot_cap = y_v.shape[2]
    pair_rows = dev_slots * slot_cap
    bufs = w_v.shape[0]
    tiles = ff // 128
    far = ring // 2
    chunks = ring - 1
    me = lax.axis_index('ep')
    pos = ring_of(me)
    ahead = (index_of(pos + 1), index_of(pos - 1))
    col_tile = min(512, hidden)

    barrier = pltpu.get_barrier_semaphore()
    for off in range(1, ring):
        pl.semaphore_signal(barrier, inc=1, device_id={'ep': index_of(pos + off)}, device_id_type=MESH)

    own_meta = pltpu.make_async_copy(meta_hbm, meta_v.at[0], own_sem.at[0])
    own_toks = [pltpu.make_async_copy(tok_hbm.at[pl.ds(sub * sub_rows, sub_rows)], tok_v.at[0, sub], tok_sem.at[sub]) for sub in (0, 1)]
    own_meta.start()
    for copy in own_toks:
        copy.start()

    def chunk(i, way):
        dist = (i + 1) // 2
        sub = (i + 1) % 2 + way * (i // chunks)
        if way == 0:
            src, dst = (ring + 1 - dist) % ring, ring - dist
        else:
            src, dst = dist - 1, dist
        return pltpu.make_async_remote_copy(
            src_ref=tok_v.at[src, sub], dst_ref=tok_v.at[dst, sub],
            send_sem=send_sem.at[way, i - 1], recv_sem=recv_sem.at[way, i - 1],
            device_id={'ep': ahead[way]}, device_id_type=MESH)

    def tick(i):
        for way in (0, 1):
            chunk(i, way).wait_recv()

            @pl.when(i <= chunks - 3)
            def _():
                chunk(i + 2, way).start()

            @pl.when(i == chunks - 2 + way)
            def _():
                chunk(chunks, way).start()

    def meta_copy(off):
        return pltpu.make_async_remote_copy(
            src_ref=meta_v.at[0], dst_ref=meta_v.at[ring - off],
            send_sem=msend_sem.at[off - 1], recv_sem=mrecv_sem.at[ring - off - 1],
            device_id={'ep': index_of(pos + off)}, device_id_type=MESH)

    def stream(copies_of, use, low, high, total):
        def body(i, _):
            for copy in copies_of(i):
                copy.wait()
            use(i, i % bufs)

            @pl.when(i + bufs < total)
            def _():
                for copy in copies_of(i + bufs):
                    copy.start()
            return 0
        lax.fori_loop(low, high, body, 0)

    def open_stream(copies_of):
        for i in range(bufs):
            for copy in copies_of(i):
                copy.start()

    def shared_copies(i):
        cols = pl.ds(pl.multiple_of(i * 128, 128), 128)
        return (pltpu.make_async_copy(shg_hbm.at[:, cols], w_v.at[i % bufs, :, pl.ds(0, 128)], w_sem.at[i % bufs, 0]),
                pltpu.make_async_copy(shu_hbm.at[:, cols], w_v.at[i % bufs, :, pl.ds(128, 128)], w_sem.at[i % bufs, 1]))

    def shared_use(i, buf):
        cols = pl.ds(pl.multiple_of(i % tiles * 128, 128), 128)
        for sub in (0, 1):
            both = jnp.dot(tok_v[0, sub], w_v[buf], preferred_element_type=jnp.float32)
            h_v[i // tiles, sub * sub_rows:(sub + 1) * sub_rows, cols] = (jax.nn.silu(both[:, :128]) * both[:, 128:]).astype(jnp.bfloat16)

    def last_copies(i):
        cols = pl.ds(pl.multiple_of(i // 2 * 256, 256), 256)
        rows = pl.ds(pl.multiple_of(i % 2 * ff, 128), ff)
        return (pltpu.make_async_copy(shd_hbm.at[rows, cols], w_v.at[i % bufs, pl.ds(0, ff), :], w_sem.at[i % bufs, 0]),)

    def z_copy(tile):
        cols = pl.ds(pl.multiple_of(tile * 256, 256), 256)
        return pltpu.make_async_copy(z_v.at[tile % 2], z_hbm.at[:, cols], z_sem.at[tile % 2])

    def last_use(i, buf):
        tile = i // 2
        part = jnp.dot(h_v[i % 2, :tok_count, :], w_v[buf, :ff, :], preferred_element_type=jnp.float32)

        @pl.when(i % 2 == 0)
        def _():
            @pl.when(tile >= 2)
            def _():
                z_copy(tile - 2).wait()
            z_v[tile % 2] = part

        @pl.when(i % 2 == 1)
        def _():
            z_v[tile % 2] += part
            z_copy(tile).start()

    def select(block, keep_rows):
        ids = (lax.broadcasted_iota(jnp.int32, (pair_rows, 1), 0) + me * pair_rows).astype(jnp.float32)
        hit = meta_v[block, 0:1, :] == ids
        for j in range(1, 6):
            hit = hit | (meta_v[block, j:j + 1, :] == ids)
        pick = hit.astype(jnp.float32).astype(jnp.bfloat16)

        def one_tile(tile, _):
            cols = pl.ds(pl.multiple_of(tile * col_tile, col_tile), col_tile)
            rows = jnp.dot(pick[:, :sub_rows], tok_v[block, 0, :, cols], preferred_element_type=jnp.float32)
            rows += jnp.dot(pick[:, sub_rows:], tok_v[block, 1, :, cols], preferred_element_type=jnp.float32)
            rows = rows.astype(jnp.bfloat16)
            for slot in range(dev_slots):
                keep_rows(slot, cols, rows[slot * slot_cap:(slot + 1) * slot_cap])
            return 0
        lax.fori_loop(0, hidden // col_tile, one_tile, 0)

    def dispatch(block, place):
        at = pl.multiple_of(place * slot_cap, 16)

        def keep_rows(slot, cols, rows):
            rows_v[slot, pl.ds(at, slot_cap), cols] = rows
        select(block, keep_rows)

    def far_copy(place):
        at = pl.ds(pl.multiple_of(place * slot_cap, 16), slot_cap)
        return pltpu.make_async_copy(far_v.at[place % 2], far_hbm.at[:, at, :], far_sem.at[place % 2])

    def far_dispatch(block, place):
        @pl.when(place >= 2)
        def _():
            far_copy(place - 2).wait()

        def keep_rows(slot, cols, rows):
            far_v[place % 2, slot, :, cols] = rows
        select(block, keep_rows)
        far_copy(place).start()

    open_slots, run_slots, close_slots, segs = slot_stream(
        gate_hbm, up_hbm, down_hbm, rows_v, w_v, h_v.at[0], y_v, y_hbm, w_sem, y_sem)

    open_stream(shared_copies)
    own_meta.wait()
    for copy in own_toks:
        copy.wait()
    pl.semaphore_wait(barrier, ring - 1)
    for off in range(1, ring):
        meta_copy(off).start()
    for i in (1, 2):
        for way in (0, 1):
            chunk(i, way).start()
    stream(shared_copies, shared_use, 0, tiles, 2 * tiles)
    tick(1)
    stream(shared_copies, shared_use, tiles, 2 * tiles, 2 * tiles)
    open_stream(last_copies)
    for off in range(1, ring):
        meta_copy(off).wait_recv()
    keep = pltpu.make_async_copy(meta_v, all_meta_hbm, keep_sem)
    keep.start()
    tick(2)
    downs = 2 * (hidden // 256)
    stream(last_copies, last_use, 0, downs, downs)
    tick(3)
    open_slots()
    for tile in (hidden // 256 - 2, hidden // 256 - 1):
        z_copy(tile).wait()
    tick(4)
    dispatch(0, 0)

    def one_pair(dist, _):
        @pl.when(dist >= 3)
        def _():
            tick(2 * dist - 1)
            tick(2 * dist)
        dispatch(ring - dist, 2 * dist - 1)
        dispatch(dist, 2 * dist)
        return 0
    lax.fori_loop(1, far // 2 + 1, one_pair, 0)
    left = chunks - far

    def one_seg(seg, _):
        @pl.when(seg < segs)
        def _():
            run_slots(seg)

        @pl.when(seg < left)
        def _():
            tick(far + 1 + seg)

        @pl.when((seg % 2 == 1) & (seg < left))
        def _():
            dist = far // 2 + 1 + seg // 2
            far_dispatch(ring - dist, seg - 1)
            far_dispatch(dist, seg)
        return 0
    lax.fori_loop(0, max(segs, left), one_seg, 0)
    far_dispatch(far, jnp.int32(far - 2))
    close_slots()
    far_copy(jnp.int32(far - 3)).wait()
    far_copy(jnp.int32(far - 2)).wait()
    keep.wait()
    for off in range(1, ring):
        meta_copy(off).wait_send()
    for i in range(1, ring):
        for way in (0, 1):
            chunk(i, way).wait_send()


def gather_rows(tok_rows, meta, w_gate, w_up, w_down, sh_gate, sh_up, sh_down, ring, slot_cap):
    tok_count, hidden = tok_rows.shape
    dev_slots, _, ff = w_gate.shape
    any_spec = pl.BlockSpec(memory_space=pl.ANY)
    dma = pltpu.SemaphoreType.DMA
    near = ring // 2 + 1
    flops = 6 * hidden * ff * near * dev_slots * slot_cap + 12 * tok_count * hidden * ff
    return pl.pallas_call(
        gather_kernel,
        out_shape=(jax.ShapeDtypeStruct((near, dev_slots * slot_cap, hidden), jnp.bfloat16),
                   jax.ShapeDtypeStruct((dev_slots, (ring - near) * slot_cap, hidden), jnp.bfloat16),
                   jax.ShapeDtypeStruct((ring,) + meta.shape, jnp.float32),
                   jax.ShapeDtypeStruct((tok_count, hidden), jnp.float32)),
        in_specs=[any_spec] * 8,
        out_specs=(any_spec,) * 4,
        scratch_shapes=[
            pltpu.VMEM((ring, 2, tok_count // 2, hidden), jnp.bfloat16),
            pltpu.VMEM((ring,) + meta.shape, jnp.float32),
            pltpu.VMEM((dev_slots, near * slot_cap, hidden), jnp.bfloat16),
            pltpu.VMEM((2, dev_slots, slot_cap, hidden), jnp.bfloat16),
            pltpu.VMEM((4, hidden, 256), jnp.bfloat16),
            pltpu.VMEM((2, near * slot_cap, ff), jnp.bfloat16),
            pltpu.VMEM((2, near, slot_cap, 256), jnp.bfloat16),
            pltpu.VMEM((2, tok_count, 256), jnp.float32),
            dma((2,)), dma((1,)), dma((4, 2)), dma((2,)), dma((2,)), dma((2,)), dma,
            dma((2, ring - 1)), dma((2, ring - 1)), dma((ring - 1,)), dma((ring - 1,)),
        ],
        compiler_params=pltpu.CompilerParams(collective_id=2, has_side_effects=True, vmem_limit_bytes=67_000_000),
        cost_estimate=pl.CostEstimate(flops=flops, bytes_accessed=170_000_000, transcendentals=0),
        name='gather_rows',
    )(tok_rows, meta, w_gate, w_up, w_down, sh_gate, sh_up, sh_down)


def reduce_kernel(near_hbm, x_hbm, meta_hbm, gate_hbm, up_hbm, down_hbm, out_hbm, far_hbm,
                  x_v, w_v, h_v, y_v, meta_v, weigh_v, tri_v, own_v, run_v,
                  x_sem, w_sem, y_sem, tri_sem, meta_sem, send_sem, recv_sem, free_sem, out_sem):
    steps = meta_hbm.shape[0]
    near = near_hbm.shape[0]
    pair_rows = near_hbm.shape[1]
    half = run_v.shape[4]
    sub_rows = run_v.shape[3]
    mix_tile = min(256, half)
    tok_tile = min(128, 2 * sub_rows)
    wide = weigh_v.shape[1] // 3
    early = near // 2
    me = lax.axis_index('ep')
    pos = ring_of(me)
    ahead = (index_of(pos + 1), index_of(pos - 1))
    behind = (index_of(pos - 1), index_of(pos + 1))

    barrier = pltpu.get_barrier_semaphore()
    for peer in ahead:
        pl.semaphore_signal(barrier, inc=1, device_id={'ep': peer}, device_id_type=MESH)

    def block_of(step, way):
        return steps - 1 - step if way == 0 else (step + 1) % steps

    def place_of(step, way):
        behind_half = (step + 1) // (steps // 2 + 1)
        dist = step + 1 + behind_half * (steps - 2 - 2 * step)
        side = way + behind_half * (1 - 2 * way)
        middle = dist // (steps // 2)
        last = (step + 1) // steps
        return (2 * dist - 1 + side) * (1 - middle) * (1 - last) + middle * (steps - 1)

    def meta_fetch(step, way):
        return pltpu.make_async_copy(meta_hbm.at[block_of(step, way)], meta_v.at[step % 2, way], meta_sem.at[step % 2, way])

    def tri_fetch(step, way, part, source, base):
        cols = pl.ds(way * half, half)
        return pltpu.make_async_copy(source.at[place_of(step, way) - base, :, cols],
                                     tri_v.at[step % 2, way, pl.ds(part * wide, pair_rows), :], tri_sem.at[step % 2, way, part])

    def wait_tri(par, way, part):
        pltpu.make_async_copy(near_hbm.at[0, :, pl.ds(way * half, half)],
                              tri_v.at[par, way, pl.ds(part * wide, pair_rows), :], tri_sem.at[par, way, part]).wait()

    def start_fetch(step, is_far):
        for way in (0, 1):
            meta_fetch(step, way).start()
            for part in range(3):
                tri_fetch(step, way, part, *((far_hbm, near) if is_far else (near_hbm, 0))).start()

    def build_weigh(par, way):
        lane = lax.broadcasted_iota(jnp.int32, (1, wide), 1)
        ids = jnp.where(lane < pair_rows, lane + me * pair_rows, -1).astype(jnp.float32)

        def one_tile(tile, _):
            toks = pl.ds(pl.multiple_of(tile * tok_tile, tok_tile), tok_tile)
            info = jnp.transpose(meta_v[par, way, :, toks])
            weigh = jnp.zeros((tok_tile, wide), jnp.float32)
            for j in range(6):
                weigh = jnp.where(info[:, j:j + 1] == ids, info[:, 6 + j:7 + j], weigh)
            hi = weigh.astype(jnp.bfloat16)
            rest = weigh - hi.astype(jnp.float32)
            mid = rest.astype(jnp.bfloat16)
            low = (rest - mid.astype(jnp.float32)).astype(jnp.bfloat16)
            weigh_v[toks, :wide] = low
            weigh_v[toks, wide:2 * wide] = mid
            weigh_v[toks, 2 * wide:] = hi
            return 0
        lax.fori_loop(0, 2 * sub_rows // tok_tile, one_tile, 0)

    def compute_own(step):
        par = step % 2
        for way in (0, 1):
            meta_fetch(step, way).wait()
            build_weigh(par, way)
            for part in range(3):
                wait_tri(par, way, part)

            def one_tile(tile, _):
                cols = pl.ds(pl.multiple_of(tile * mix_tile, mix_tile), mix_tile)
                own_v[way, :, cols] = jnp.dot(weigh_v[...], tri_v[par, way, :, cols], preferred_element_type=jnp.float32)
                return 0

            lax.fori_loop(0, half // mix_tile, one_tile, 0)

    def send(step, way, sub):
        now, later = step % 2, (step + 1) % 2
        return pltpu.make_async_remote_copy(
            src_ref=run_v.at[way, now, sub], dst_ref=run_v.at[way, later, sub],
            send_sem=send_sem.at[way, now, sub], recv_sem=recv_sem.at[way, later, sub],
            device_id={'ep': ahead[way]}, device_id_type=MESH)

    open_slots, run_slots, close_slots, segs = slot_stream(
        gate_hbm, up_hbm, down_hbm, x_v, w_v, h_v, y_v, far_hbm, w_sem, y_sem)
    per_step = -(-segs // (2 * early))

    for par in (0, 1):
        for way in (0, 1):
            for part in range(3):
                tri_v[par, way, part * wide + pair_rows:(part + 1) * wide, :] = jnp.zeros((wide - pair_rows, half), jnp.bfloat16)
    start_fetch(0, False)
    start_fetch(1, False)
    x_copy = pltpu.make_async_copy(x_hbm, x_v, x_sem)
    x_copy.start()
    open_slots()
    compute_own(0)
    start_fetch(2, False)
    pl.semaphore_wait(barrier, 2)
    for sub in (0, 1):
        for way in (0, 1):
            run_v[way, 0, sub] = own_v[way, sub * sub_rows:(sub + 1) * sub_rows, :]
            send(0, way, sub).start()
    x_copy.wait()

    def far_work(step, sub):
        for more in range(per_step):
            run_slots((2 * step + sub) * per_step + more)

    far_work(0, 0)
    compute_own(1)
    start_fetch(3, False)
    far_work(0, 1)

    def pass_on(step, sub):
        now = step % 2
        for way in (0, 1):
            send(step - 1, way, sub).wait_recv()
            send(step - 1, way, sub).wait_send()
            pl.semaphore_signal(free_sem.at[way, sub], inc=1, device_id={'ep': behind[way]}, device_id_type=MESH)
            run_v[way, now, sub] += own_v[way, sub * sub_rows:(sub + 1) * sub_rows, :]
            pl.semaphore_wait(free_sem.at[way, sub], 1)
            send(step, way, sub).start()

    def early_step(step, _):
        pass_on(step, 0)
        far_work(step, 0)
        pass_on(step, 1)
        far_work(step, 1)

        @pl.when(step == early - 1)
        def _():
            close_slots()
            start_fetch(early, True)
            start_fetch(early + 1, True)
        compute_own(step + 1)
        return 0

    lax.fori_loop(1, early, early_step, 0)
    start_fetch(early + 2, True)

    def late_step(step, _):
        pass_on(step, 0)
        pass_on(step, 1)
        compute_own(step + 1)
        ahead_far = step + 3 < steps - 1 - early

        @pl.when(ahead_far)
        def _():
            start_fetch(step + 3, True)

        @pl.when(jnp.logical_not(ahead_far) & (step + 3 < steps))
        def _():
            start_fetch(step + 3, False)
        return 0

    lax.fori_loop(early, steps - 1, late_step, 0)
    last = (steps - 1) % 2
    outs = []
    for sub in (0, 1):
        for way in (0, 1):
            send(steps - 2, way, sub).wait_recv()
            send(steps - 2, way, sub).wait_send()
            run_v[way, last, sub] += own_v[way, sub * sub_rows:(sub + 1) * sub_rows, :]
            outs.append(pltpu.make_async_copy(run_v.at[way, last, sub],
                                              out_hbm.at[pl.ds(sub * sub_rows, sub_rows), pl.ds(way * half, half)],
                                              out_sem.at[way, sub]))
            outs[-1].start()
    for copy in outs:
        copy.wait()


def reduce_home(near_out, far_rows, meta, w_gate, w_up, w_down):
    near, pair_rows, hidden = near_out.shape
    dev_slots, ff, _ = w_down.shape
    slot_cap = pair_rows // dev_slots
    steps, _, tok_count = meta.shape
    far = steps - near
    half, sub_rows = hidden // 2, tok_count // 2
    wide = (pair_rows + 127) // 128 * 128
    any_spec = pl.BlockSpec(memory_space=pl.ANY)
    dma = pltpu.SemaphoreType.DMA
    flops = 6 * far * pair_rows * hidden * ff + 6 * steps * pair_rows * hidden * tok_count
    return pl.pallas_call(
        reduce_kernel,
        out_shape=(jax.ShapeDtypeStruct((tok_count, hidden), jnp.float32),
                   jax.ShapeDtypeStruct((far, pair_rows, hidden), jnp.bfloat16)),
        in_specs=[any_spec] * 6,
        out_specs=(any_spec,) * 2,
        scratch_shapes=[
            pltpu.VMEM((dev_slots, far * slot_cap, hidden), jnp.bfloat16),
            pltpu.VMEM((4, hidden, 256), jnp.bfloat16),
            pltpu.VMEM((far * slot_cap, ff), jnp.bfloat16),
            pltpu.VMEM((2, far, slot_cap, 256), jnp.bfloat16),
            pltpu.VMEM((2, 2) + meta.shape[1:], jnp.float32),
            pltpu.VMEM((tok_count, 3 * wide), jnp.bfloat16),
            pltpu.VMEM((2, 2, 3 * wide, half), jnp.bfloat16),
            pltpu.VMEM((2, tok_count, half), jnp.float32),
            pltpu.VMEM((2, 2, 2, sub_rows, half), jnp.float32),
            dma, dma((4, 2)), dma((2,)), dma((2, 2, 3)), dma((2, 2)), dma((2, 2, 2)), dma((2, 2, 2)),
            pltpu.SemaphoreType.REGULAR((2, 2)), dma((2, 2)),
        ],
        compiler_params=pltpu.CompilerParams(collective_id=1, has_side_effects=True, vmem_limit_bytes=65_000_000),
        cost_estimate=pl.CostEstimate(flops=flops, bytes_accessed=170_000_000, transcendentals=0),
        name='reduce_home',
    )(near_out, far_rows, meta, w_gate, w_up, w_down)[0]


def solution(mesh):
    ep_size = mesh.shape['ep']

    def local_block(tok_rows, router_w, top_idx, slot_idx, w_gate, w_up, w_down, sh_gate, sh_up, sh_down):
        tok_count = tok_rows.shape[0]
        top_k = top_idx.shape[1]
        dev_slots = w_gate.shape[0]
        num_slots = ep_size * dev_slots
        slot_cap = ((2 * tok_count * top_k + num_slots - 1) // num_slots + 15) // 16 * 16
        logits = jnp.dot(tok_rows, router_w, preferred_element_type=jnp.float32)
        scores = jax.nn.sigmoid(logits)
        exp_ids = jnp.arange(router_w.shape[1], dtype=jnp.int32)
        picked = jnp.sum(jnp.where(top_idx[:, :, None] == exp_ids, scores[:, None, :], 0.0), axis=2)
        gate_wts = picked / jnp.sum(picked, axis=1, keepdims=True) * ROUTE_SCALE
        match = slot_idx[:, :, None] == jnp.arange(num_slots, dtype=jnp.int32)
        hot = jnp.any(match, axis=1)
        before = (jnp.arange(tok_count)[:, None] > jnp.arange(tok_count)[None, :]).astype(jnp.bfloat16)
        rank = jnp.dot(before, hot.astype(jnp.bfloat16), preferred_element_type=jnp.float32)
        dest = slot_idx.astype(jnp.float32) * slot_cap + jnp.sum(jnp.where(match, rank[:, None, :], 0.0), axis=2)
        meta = jnp.concatenate([dest, gate_wts, jnp.zeros((tok_count, 16 - 2 * top_k), jnp.float32)], axis=1).T
        near_out, far_rows, all_meta, shared_out = gather_rows(tok_rows, meta, w_gate, w_up, w_down, sh_gate, sh_up, sh_down, ep_size, slot_cap)
        routed = reduce_home(near_out, far_rows, all_meta, w_gate, w_up, w_down)
        return (shared_out + routed).astype(jnp.bfloat16)

    tok_spec = P(('dp', 'ep'), None)
    slot_spec = P('ep', None, None)
    return jax.shard_map(local_block, mesh=mesh,
                         in_specs=(tok_spec, P(None, None), tok_spec, tok_spec, slot_spec, slot_spec, slot_spec,
                                   P(None, None), P(None, None), P(None, None)),
                         out_specs=tok_spec, check_vma=False)
```

```python
import functools

import jax
import jax.numpy as jnp
from jax import lax
from jax.experimental import pallas as pl
from jax.experimental.pallas import tpu as pltpu
from jax.sharding import PartitionSpec as P

ROUTE_SCALE = 2.5
MESH = pl.DeviceIdType.MESH


def ring_of(idx):
    z, y, core = idx // 4, (idx // 2) % 2, idx % 2
    return (z + y * (7 - 2 * z)) * 2 + core


def index_of(pos):
    pos = (pos + 32) % 16
    chip, core = pos // 2, pos % 2
    back = chip // 4
    z = chip + back * (7 - 2 * chip)
    return z * 4 + back * 2 + core


SEG = 12


def slot_stream(gate_hbm, up_hbm, down_hbm, rows_v, w_v, g_v, h_v, y_v, y_hbm, w_sem, y_sem):
    dev_slots, rows = rows_v.shape[:2]
    ff = h_v.shape[1]
    bufs = w_v.shape[0]
    whole = ff // 256 * 2
    ups, downs = ff // 128, rows_v.shape[2] // 256
    per_slot = ups + downs
    total = dev_slots * per_slot
    slot_cap = y_v.shape[2]

    def wide_copy(i, weight_hbm):
        slot, tile = i // per_slot, i % per_slot
        cols = pl.ds(pl.multiple_of(tile // 2 * 256, 256), 256)
        return pltpu.make_async_copy(weight_hbm.at[slot, :, cols], w_v.at[i % bufs], w_sem.at[i % bufs, 0])

    def pair_copies(i):
        slot = i // per_slot
        cols = pl.ds(whole * 128, 128)
        return (pltpu.make_async_copy(gate_hbm.at[slot, :, cols], w_v.at[i % bufs, :, pl.ds(0, 128)], w_sem.at[i % bufs, 0]),
                pltpu.make_async_copy(up_hbm.at[slot, :, cols], w_v.at[i % bufs, :, pl.ds(128, 128)], w_sem.at[i % bufs, 1]))

    def down_copies(i):
        slot, tile = i // per_slot, i % per_slot - ups
        cols = pl.ds(pl.multiple_of(tile * 256, 256), 256)
        return [pltpu.make_async_copy(down_hbm.at[slot, pl.ds(part * (ff // 2), ff // 2), cols],
                                      w_v.at[i % bufs, pl.ds(part * (ff // 2), ff // 2), :], w_sem.at[i % bufs, part]) for part in (0, 1)]

    def fetch(i):
        @pl.when((i % per_slot < whole) & (i % per_slot % 2 == 0))
        def _():
            wide_copy(i, gate_hbm).start()

        @pl.when((i % per_slot < whole) & (i % per_slot % 2 == 1))
        def _():
            wide_copy(i, up_hbm).start()

        if whole < ups:
            @pl.when(i % per_slot == whole)
            def _():
                for copy in pair_copies(i):
                    copy.start()

        @pl.when(i % per_slot >= ups)
        def _():
            for copy in down_copies(i):
                copy.start()

    def y_copy(slot, tile):
        cols = pl.ds(pl.multiple_of(tile * 256, 256), 256)
        at = pl.ds(pl.multiple_of(slot * slot_cap, 16), slot_cap)
        return pltpu.make_async_copy(y_v.at[tile % 2], y_hbm.at[:, at, cols], y_sem.at[tile % 2])

    def one(i, _):
        slot, k, buf = i // per_slot, i % per_slot, i % bufs

        @pl.when((k < whole) & (k % 2 == 0))
        def _():
            wide_copy(i, gate_hbm).wait()
            g_v[...] = jnp.dot(rows_v[slot], w_v[buf], preferred_element_type=jnp.float32)

        @pl.when((k < whole) & (k % 2 == 1))
        def _():
            wide_copy(i, up_hbm).wait()
            up_act = jnp.dot(rows_v[slot], w_v[buf], preferred_element_type=jnp.float32)
            cols = pl.ds(pl.multiple_of(k // 2 * 256, 256), 256)
            h_v[:rows, cols] = (jax.nn.silu(g_v[...]) * up_act).astype(jnp.bfloat16)

        if whole < ups:
            @pl.when(k == whole)
            def _():
                for copy in pair_copies(i):
                    copy.wait()
                both = jnp.dot(rows_v[slot], w_v[buf], preferred_element_type=jnp.float32)
                h_v[:rows, whole * 128:] = (jax.nn.silu(both[:, :128]) * both[:, 128:]).astype(jnp.bfloat16)

        @pl.when(k >= ups)
        def _():
            for copy in down_copies(i):
                copy.wait()
            tile = k - ups

            @pl.when((slot > 0) | (tile >= 2))
            def _():
                y_copy(slot, tile).wait()
            outs = jnp.dot(h_v[:rows, :], w_v[buf, :ff, :], preferred_element_type=jnp.float32).astype(jnp.bfloat16)
            y_v[tile % 2] = outs.reshape(rows // slot_cap, slot_cap, 256)
            y_copy(slot, tile).start()

        @pl.when(i + bufs < total)
        def _():
            fetch(i + bufs)
        return 0

    def open_all():
        for i in range(bufs):
            fetch(jnp.int32(i))

    def run(seg):
        lax.fori_loop(seg * SEG, jnp.minimum(seg * SEG + SEG, total), one, 0)

    def close():
        for tile in (downs - 2, downs - 1):
            y_copy(dev_slots - 1, tile).wait()

    return open_all, run, close, -(-total // SEG)


def gather_kernel(tok_hbm, meta_hbm, gate_hbm, up_hbm, down_hbm, shg_hbm, shu_hbm, shd_hbm, y_hbm, far_hbm, all_meta_hbm, z_hbm,
                  tok_v, meta_v, rows_v, far_v, w_v, g_v, h_v, y_v, z_v,
                  tok_sem, own_sem, w_sem, y_sem, far_sem, z_sem, keep_sem, send_sem, recv_sem, msend_sem, mrecv_sem):
    ring, _, sub_rows, hidden = tok_v.shape
    dev_slots = rows_v.shape[0]
    ff = h_v.shape[2]
    tok_count = 2 * sub_rows
    slot_cap = y_v.shape[2]
    pair_rows = dev_slots * slot_cap
    bufs = w_v.shape[0]
    tiles = ff // 128
    far = ring // 2
    chunks = ring - 1
    me = lax.axis_index('ep')
    pos = ring_of(me)
    ahead = (index_of(pos + 1), index_of(pos - 1))
    col_tile = min(512, hidden)

    barrier = pltpu.get_barrier_semaphore()
    for off in range(1, ring):
        pl.semaphore_signal(barrier, inc=1, device_id={'ep': index_of(pos + off)}, device_id_type=MESH)

    own_meta = pltpu.make_async_copy(meta_hbm, meta_v.at[0], own_sem.at[0])
    own_toks = [pltpu.make_async_copy(tok_hbm.at[pl.ds(sub * sub_rows, sub_rows)], tok_v.at[0, sub], tok_sem.at[sub]) for sub in (0, 1)]
    own_meta.start()
    for copy in own_toks:
        copy.start()

    def chunk(i, way):
        dist = (i + 1) // 2
        sub = (i + 1) % 2 + way * (i // chunks)
        if way == 0:
            src, dst = (ring + 1 - dist) % ring, ring - dist
        else:
            src, dst = dist - 1, dist
        return pltpu.make_async_remote_copy(
            src_ref=tok_v.at[src, sub], dst_ref=tok_v.at[dst, sub],
            send_sem=send_sem.at[way, i - 1], recv_sem=recv_sem.at[way, i - 1],
            device_id={'ep': ahead[way]}, device_id_type=MESH)

    def tick(i):
        for way in (0, 1):
            chunk(i, way).wait_recv()

            @pl.when(i <= chunks - 3)
            def _():
                chunk(i + 2, way).start()

            @pl.when(i == chunks - 2 + way)
            def _():
                chunk(chunks, way).start()

    def meta_copy(off):
        return pltpu.make_async_remote_copy(
            src_ref=meta_v.at[0], dst_ref=meta_v.at[ring - off],
            send_sem=msend_sem.at[off - 1], recv_sem=mrecv_sem.at[ring - off - 1],
            device_id={'ep': index_of(pos + off)}, device_id_type=MESH)

    def stream(copies_of, use, low, high, total):
        def body(i, _):
            for copy in copies_of(i):
                copy.wait()
            use(i, i % bufs)

            @pl.when(i + bufs < total)
            def _():
                for copy in copies_of(i + bufs):
                    copy.start()
            return 0
        lax.fori_loop(low, high, body, 0)

    def open_stream(copies_of):
        for i in range(bufs):
            for copy in copies_of(i):
                copy.start()

    def shared_copies(i):
        cols = pl.ds(pl.multiple_of(i * 128, 128), 128)
        return (pltpu.make_async_copy(shg_hbm.at[:, cols], w_v.at[i % bufs, :, pl.ds(0, 128)], w_sem.at[i % bufs, 0]),
                pltpu.make_async_copy(shu_hbm.at[:, cols], w_v.at[i % bufs, :, pl.ds(128, 128)], w_sem.at[i % bufs, 1]))

    def shared_use(i, buf):
        cols = pl.ds(pl.multiple_of(i % tiles * 128, 128), 128)
        for sub in (0, 1):
            both = jnp.dot(tok_v[0, sub], w_v[buf], preferred_element_type=jnp.float32)
            h_v[i // tiles, sub * sub_rows:(sub + 1) * sub_rows, cols] = (jax.nn.silu(both[:, :128]) * both[:, 128:]).astype(jnp.bfloat16)

    def last_copies(i):
        cols = pl.ds(pl.multiple_of(i // 2 * 256, 256), 256)
        rows = pl.ds(pl.multiple_of(i % 2 * ff, 128), ff)
        return (pltpu.make_async_copy(shd_hbm.at[rows, cols], w_v.at[i % bufs, pl.ds(0, ff), :], w_sem.at[i % bufs, 0]),)

    def z_copy(tile):
        cols = pl.ds(pl.multiple_of(tile * 256, 256), 256)
        return pltpu.make_async_copy(z_v.at[tile % 2], z_hbm.at[:, cols], z_sem.at[tile % 2])

    def last_use(i, buf):
        tile = i // 2
        part = jnp.dot(h_v[i % 2, :tok_count, :], w_v[buf, :ff, :], preferred_element_type=jnp.float32)

        @pl.when(i % 2 == 0)
        def _():
            @pl.when(tile >= 2)
            def _():
                z_copy(tile - 2).wait()
            z_v[tile % 2] = part

        @pl.when(i % 2 == 1)
        def _():
            z_v[tile % 2] += part
            z_copy(tile).start()

    def select(block, keep_rows):
        ids = (lax.broadcasted_iota(jnp.int32, (pair_rows, 1), 0) + me * pair_rows).astype(jnp.float32)
        hit = meta_v[block, 0:1, :] == ids
        for j in range(1, 6):
            hit = hit | (meta_v[block, j:j + 1, :] == ids)
        pick = hit.astype(jnp.float32).astype(jnp.bfloat16)

        def one_tile(tile, _):
            cols = pl.ds(pl.multiple_of(tile * col_tile, col_tile), col_tile)
            rows = jnp.dot(pick[:, :sub_rows], tok_v[block, 0, :, cols], preferred_element_type=jnp.float32)
            rows += jnp.dot(pick[:, sub_rows:], tok_v[block, 1, :, cols], preferred_element_type=jnp.float32)
            rows = rows.astype(jnp.bfloat16)
            for slot in range(dev_slots):
                keep_rows(slot, cols, rows[slot * slot_cap:(slot + 1) * slot_cap])
            return 0
        lax.fori_loop(0, hidden // col_tile, one_tile, 0)

    def dispatch(block, place):
        at = pl.multiple_of(place * slot_cap, 16)

        def keep_rows(slot, cols, rows):
            rows_v[slot, pl.ds(at, slot_cap), cols] = rows
        select(block, keep_rows)

    def far_copy(place):
        at = pl.ds(pl.multiple_of(place * slot_cap, 16), slot_cap)
        return pltpu.make_async_copy(far_v.at[place % 2], far_hbm.at[:, at, :], far_sem.at[place % 2])

    def far_dispatch(block, place):
        @pl.when(place >= 2)
        def _():
            far_copy(place - 2).wait()

        def keep_rows(slot, cols, rows):
            far_v[place % 2, slot, :, cols] = rows
        select(block, keep_rows)
        far_copy(place).start()

    open_slots, run_slots, close_slots, segs = slot_stream(
        gate_hbm, up_hbm, down_hbm, rows_v, w_v, g_v, h_v.at[0], y_v, y_hbm, w_sem, y_sem)

    open_stream(shared_copies)
    own_meta.wait()
    for copy in own_toks:
        copy.wait()
    pl.semaphore_wait(barrier, ring - 1)
    for off in range(1, ring):
        meta_copy(off).start()
    for i in (1, 2):
        for way in (0, 1):
            chunk(i, way).start()
    stream(shared_copies, shared_use, 0, tiles, 2 * tiles)
    tick(1)
    stream(shared_copies, shared_use, tiles, 2 * tiles, 2 * tiles)
    open_stream(last_copies)
    for off in range(1, ring):
        meta_copy(off).wait_recv()
    keep = pltpu.make_async_copy(meta_v, all_meta_hbm, keep_sem)
    keep.start()
    tick(2)
    downs = 2 * (hidden // 256)
    stream(last_copies, last_use, 0, downs, downs)
    tick(3)
    open_slots()
    for tile in (hidden // 256 - 2, hidden // 256 - 1):
        z_copy(tile).wait()
    tick(4)
    dispatch(0, 0)

    def one_pair(dist, _):
        @pl.when(dist >= 3)
        def _():
            tick(2 * dist - 1)
            tick(2 * dist)
        dispatch(ring - dist, 2 * dist - 1)
        dispatch(dist, 2 * dist)
        return 0
    lax.fori_loop(1, far // 2 + 1, one_pair, 0)
    left = chunks - far

    def one_seg(seg, _):
        @pl.when(seg < segs)
        def _():
            run_slots(seg)

        @pl.when(seg < left)
        def _():
            tick(far + 1 + seg)

        @pl.when((seg % 2 == 1) & (seg < left))
        def _():
            dist = far // 2 + 1 + seg // 2
            far_dispatch(ring - dist, seg - 1)
            far_dispatch(dist, seg)
        return 0
    lax.fori_loop(0, max(segs, left), one_seg, 0)
    far_dispatch(far, jnp.int32(far - 2))
    close_slots()
    far_copy(jnp.int32(far - 3)).wait()
    far_copy(jnp.int32(far - 2)).wait()
    keep.wait()
    for off in range(1, ring):
        meta_copy(off).wait_send()
    for i in range(1, ring):
        for way in (0, 1):
            chunk(i, way).wait_send()


def gather_rows(tok_rows, meta, w_gate, w_up, w_down, sh_gate, sh_up, sh_down, ring, slot_cap):
    tok_count, hidden = tok_rows.shape
    dev_slots, _, ff = w_gate.shape
    any_spec = pl.BlockSpec(memory_space=pl.ANY)
    dma = pltpu.SemaphoreType.DMA
    near = ring // 2 + 1
    flops = 6 * hidden * ff * near * dev_slots * slot_cap + 12 * tok_count * hidden * ff
    return pl.pallas_call(
        gather_kernel,
        out_shape=(jax.ShapeDtypeStruct((near, dev_slots * slot_cap, hidden), jnp.bfloat16),
                   jax.ShapeDtypeStruct((dev_slots, (ring - near) * slot_cap, hidden), jnp.bfloat16),
                   jax.ShapeDtypeStruct((ring,) + meta.shape, jnp.float32),
                   jax.ShapeDtypeStruct((tok_count, hidden), jnp.float32)),
        in_specs=[any_spec] * 8,
        out_specs=(any_spec,) * 4,
        scratch_shapes=[
            pltpu.VMEM((ring, 2, tok_count // 2, hidden), jnp.bfloat16),
            pltpu.VMEM((ring,) + meta.shape, jnp.float32),
            pltpu.VMEM((dev_slots, near * slot_cap, hidden), jnp.bfloat16),
            pltpu.VMEM((2, dev_slots, slot_cap, hidden), jnp.bfloat16),
            pltpu.VMEM((4, hidden, 256), jnp.bfloat16),
            pltpu.VMEM((near * slot_cap, 256), jnp.float32),
            pltpu.VMEM((2, near * slot_cap, ff), jnp.bfloat16),
            pltpu.VMEM((2, near, slot_cap, 256), jnp.bfloat16),
            pltpu.VMEM((2, tok_count, 256), jnp.float32),
            dma((2,)), dma((1,)), dma((4, 2)), dma((2,)), dma((2,)), dma((2,)), dma,
            dma((2, ring - 1)), dma((2, ring - 1)), dma((ring - 1,)), dma((ring - 1,)),
        ],
        compiler_params=pltpu.CompilerParams(collective_id=2, has_side_effects=True, vmem_limit_bytes=67_000_000),
        cost_estimate=pl.CostEstimate(flops=flops, bytes_accessed=170_000_000, transcendentals=0),
        name='gather_rows',
    )(tok_rows, meta, w_gate, w_up, w_down, sh_gate, sh_up, sh_down)


def reduce_kernel(near_hbm, x_hbm, meta_hbm, z_hbm, gate_hbm, up_hbm, down_hbm, out_hbm, far_hbm,
                  z_v, x_v, w_v, g_v, h_v, y_v, meta_v, weigh_v, tri_v, own_v, run_v,
                  z_sem, x_sem, w_sem, y_sem, tri_sem, meta_sem, send_sem, recv_sem, free_sem, out_sem):
    steps = meta_hbm.shape[0]
    near = near_hbm.shape[0]
    pair_rows = near_hbm.shape[1]
    half = run_v.shape[4]
    sub_rows = run_v.shape[3]
    mix_tile = min(256, half)
    tok_tile = min(128, 2 * sub_rows)
    wide = weigh_v.shape[1] // 3
    early = near // 2
    me = lax.axis_index('ep')
    pos = ring_of(me)
    ahead = (index_of(pos + 1), index_of(pos - 1))
    behind = (index_of(pos - 1), index_of(pos + 1))

    barrier = pltpu.get_barrier_semaphore()
    for peer in ahead:
        pl.semaphore_signal(barrier, inc=1, device_id={'ep': peer}, device_id_type=MESH)

    def block_of(step, way):
        return steps - 1 - step if way == 0 else (step + 1) % steps

    def place_of(step, way):
        behind_half = (step + 1) // (steps // 2 + 1)
        dist = step + 1 + behind_half * (steps - 2 - 2 * step)
        side = way + behind_half * (1 - 2 * way)
        middle = dist // (steps // 2)
        last = (step + 1) // steps
        return (2 * dist - 1 + side) * (1 - middle) * (1 - last) + middle * (steps - 1)

    def meta_fetch(step, way):
        return pltpu.make_async_copy(meta_hbm.at[block_of(step, way)], meta_v.at[step % 2, way], meta_sem.at[step % 2, way])

    def tri_fetch(step, way, part, source, base):
        cols = pl.ds(way * half, half)
        return pltpu.make_async_copy(source.at[place_of(step, way) - base, :, cols],
                                     tri_v.at[step % 2, way, pl.ds(part * wide, pair_rows), :], tri_sem.at[step % 2, way, part])

    def wait_tri(par, way, part):
        pltpu.make_async_copy(near_hbm.at[0, :, pl.ds(way * half, half)],
                              tri_v.at[par, way, pl.ds(part * wide, pair_rows), :], tri_sem.at[par, way, part]).wait()

    def start_fetch(step, is_far):
        for way in (0, 1):
            meta_fetch(step, way).start()
            for part in range(3):
                tri_fetch(step, way, part, *((far_hbm, near) if is_far else (near_hbm, 0))).start()

    def build_weigh(par, way):
        lane = lax.broadcasted_iota(jnp.int32, (1, wide), 1)
        ids = jnp.where(lane < pair_rows, lane + me * pair_rows, -1).astype(jnp.float32)

        def one_tile(tile, _):
            toks = pl.ds(pl.multiple_of(tile * tok_tile, tok_tile), tok_tile)
            info = jnp.transpose(meta_v[par, way, :, toks])
            weigh = jnp.zeros((tok_tile, wide), jnp.float32)
            for j in range(6):
                weigh = jnp.where(info[:, j:j + 1] == ids, info[:, 6 + j:7 + j], weigh)
            hi = weigh.astype(jnp.bfloat16)
            rest = weigh - hi.astype(jnp.float32)
            mid = rest.astype(jnp.bfloat16)
            low = (rest - mid.astype(jnp.float32)).astype(jnp.bfloat16)
            weigh_v[toks, :wide] = low
            weigh_v[toks, wide:2 * wide] = mid
            weigh_v[toks, 2 * wide:] = hi
            return 0
        lax.fori_loop(0, 2 * sub_rows // tok_tile, one_tile, 0)

    def compute_own(step):
        par = step % 2
        for way in (0, 1):
            meta_fetch(step, way).wait()
            build_weigh(par, way)
            for part in range(3):
                wait_tri(par, way, part)

            def one_tile(tile, _):
                cols = pl.ds(pl.multiple_of(tile * mix_tile, mix_tile), mix_tile)
                own_v[way, :, cols] = jnp.dot(weigh_v[...], tri_v[par, way, :, cols], preferred_element_type=jnp.float32)
                return 0

            lax.fori_loop(0, half // mix_tile, one_tile, 0)

    def send(step, way, sub):
        now, later = step % 2, (step + 1) % 2
        return pltpu.make_async_remote_copy(
            src_ref=run_v.at[way, now, sub], dst_ref=run_v.at[way, later, sub],
            send_sem=send_sem.at[way, now, sub], recv_sem=recv_sem.at[way, later, sub],
            device_id={'ep': ahead[way]}, device_id_type=MESH)

    open_slots, run_slots, close_slots, segs = slot_stream(
        gate_hbm, up_hbm, down_hbm, x_v, w_v, g_v, h_v, y_v, far_hbm, w_sem, y_sem)
    per_step = -(-segs // (2 * early))

    for par in (0, 1):
        for way in (0, 1):
            for part in range(3):
                tri_v[par, way, part * wide + pair_rows:(part + 1) * wide, :] = jnp.zeros((wide - pair_rows, half), jnp.bfloat16)
    start_fetch(0, False)
    start_fetch(1, False)
    x_copy = pltpu.make_async_copy(x_hbm, x_v, x_sem)
    x_copy.start()
    open_slots()
    compute_own(0)
    start_fetch(2, False)
    pl.semaphore_wait(barrier, 2)
    for sub in (0, 1):
        for way in (0, 1):
            run_v[way, 0, sub] = own_v[way, sub * sub_rows:(sub + 1) * sub_rows, :]
            send(0, way, sub).start()
    x_copy.wait()

    def far_work(step, sub):
        for more in range(per_step):
            run_slots((2 * step + sub) * per_step + more)

    far_work(0, 0)
    compute_own(1)
    start_fetch(3, False)
    far_work(0, 1)

    def pass_on(step, sub):
        now = step % 2
        for way in (0, 1):
            send(step - 1, way, sub).wait_recv()
            send(step - 1, way, sub).wait_send()
            pl.semaphore_signal(free_sem.at[way, sub], inc=1, device_id={'ep': behind[way]}, device_id_type=MESH)
            run_v[way, now, sub] += own_v[way, sub * sub_rows:(sub + 1) * sub_rows, :]
            pl.semaphore_wait(free_sem.at[way, sub], 1)
            send(step, way, sub).start()

    def early_step(step, _):
        pass_on(step, 0)
        far_work(step, 0)
        pass_on(step, 1)
        far_work(step, 1)

        @pl.when(step == early - 1)
        def _():
            close_slots()
            start_fetch(early, True)
            start_fetch(early + 1, True)
        compute_own(step + 1)
        return 0

    lax.fori_loop(1, early, early_step, 0)
    start_fetch(early + 2, True)

    def late_step(step, _):
        pass_on(step, 0)
        pass_on(step, 1)
        compute_own(step + 1)
        ahead_far = step + 3 < steps - 1 - early

        @pl.when(ahead_far)
        def _():
            start_fetch(step + 3, True)

        @pl.when(jnp.logical_not(ahead_far) & (step + 3 < steps))
        def _():
            start_fetch(step + 3, False)
        return 0

    z_copy = pltpu.make_async_copy(z_hbm, z_v, z_sem)
    z_copy.start()
    lax.fori_loop(early, steps - 1, late_step, 0)
    z_copy.wait()
    last = (steps - 1) % 2
    outs = []
    for sub in (0, 1):
        for way in (0, 1):
            send(steps - 2, way, sub).wait_recv()
            send(steps - 2, way, sub).wait_send()
            toks = slice(sub * sub_rows, (sub + 1) * sub_rows)
            total = z_v[toks, way * half:(way + 1) * half] + (run_v[way, last, sub] + own_v[way, toks, :])
            tri_v[1 - last, way, toks, :] = total.astype(jnp.bfloat16)
            outs.append(pltpu.make_async_copy(tri_v.at[1 - last, way, pl.ds(sub * sub_rows, sub_rows), :],
                                              out_hbm.at[pl.ds(sub * sub_rows, sub_rows), pl.ds(way * half, half)],
                                              out_sem.at[way, sub]))
            outs[-1].start()
    for copy in outs:
        copy.wait()


def reduce_home(near_out, far_rows, meta, shared_out, w_gate, w_up, w_down):
    near, pair_rows, hidden = near_out.shape
    dev_slots, ff, _ = w_down.shape
    slot_cap = pair_rows // dev_slots
    steps, _, tok_count = meta.shape
    far = steps - near
    half, sub_rows = hidden // 2, tok_count // 2
    wide = (pair_rows + 127) // 128 * 128
    any_spec = pl.BlockSpec(memory_space=pl.ANY)
    dma = pltpu.SemaphoreType.DMA
    flops = 6 * far * pair_rows * hidden * ff + 6 * steps * pair_rows * hidden * tok_count
    return pl.pallas_call(
        reduce_kernel,
        out_shape=(jax.ShapeDtypeStruct((tok_count, hidden), jnp.bfloat16),
                   jax.ShapeDtypeStruct((far, pair_rows, hidden), jnp.bfloat16)),
        in_specs=[any_spec] * 7,
        out_specs=(any_spec,) * 2,
        scratch_shapes=[
            pltpu.VMEM((tok_count, hidden), jnp.float32),
            pltpu.VMEM((dev_slots, far * slot_cap, hidden), jnp.bfloat16),
            pltpu.VMEM((4, hidden, 256), jnp.bfloat16),
            pltpu.VMEM((far * slot_cap, 256), jnp.float32),
            pltpu.VMEM((far * slot_cap, ff), jnp.bfloat16),
            pltpu.VMEM((2, far, slot_cap, 256), jnp.bfloat16),
            pltpu.VMEM((2, 2) + meta.shape[1:], jnp.float32),
            pltpu.VMEM((tok_count, 3 * wide), jnp.bfloat16),
            pltpu.VMEM((2, 2, 3 * wide, half), jnp.bfloat16),
            pltpu.VMEM((2, tok_count, half), jnp.float32),
            pltpu.VMEM((2, 2, 2, sub_rows, half), jnp.float32),
            dma, dma, dma((4, 2)), dma((2,)), dma((2, 2, 3)), dma((2, 2)), dma((2, 2, 2)), dma((2, 2, 2)),
            pltpu.SemaphoreType.REGULAR((2, 2)), dma((2, 2)),
        ],
        compiler_params=pltpu.CompilerParams(collective_id=1, has_side_effects=True, vmem_limit_bytes=65_000_000),
        cost_estimate=pl.CostEstimate(flops=flops, bytes_accessed=170_000_000, transcendentals=0),
        name='reduce_home',
    )(near_out, far_rows, meta, shared_out, w_gate, w_up, w_down)[0]


def solution(mesh):
    ep_size = mesh.shape['ep']

    def local_block(tok_rows, router_w, top_idx, slot_idx, w_gate, w_up, w_down, sh_gate, sh_up, sh_down):
        tok_count = tok_rows.shape[0]
        top_k = top_idx.shape[1]
        dev_slots = w_gate.shape[0]
        num_slots = ep_size * dev_slots
        slot_cap = ((2 * tok_count * top_k + num_slots - 1) // num_slots + 15) // 16 * 16
        logits = jnp.dot(tok_rows, router_w, preferred_element_type=jnp.float32)
        scores = jax.nn.sigmoid(logits)
        exp_ids = jnp.arange(router_w.shape[1], dtype=jnp.int32)
        picked = jnp.sum(jnp.where(top_idx[:, :, None] == exp_ids, scores[:, None, :], 0.0), axis=2)
        gate_wts = picked / jnp.sum(picked, axis=1, keepdims=True) * ROUTE_SCALE
        match = slot_idx[:, :, None] == jnp.arange(num_slots, dtype=jnp.int32)
        hot = jnp.any(match, axis=1)
        before = (jnp.arange(tok_count)[:, None] > jnp.arange(tok_count)[None, :]).astype(jnp.bfloat16)
        rank = jnp.dot(before, hot.astype(jnp.bfloat16), preferred_element_type=jnp.float32)
        dest = slot_idx.astype(jnp.float32) * slot_cap + jnp.sum(jnp.where(match, rank[:, None, :], 0.0), axis=2)
        meta = jnp.concatenate([dest, gate_wts, jnp.zeros((tok_count, 16 - 2 * top_k), jnp.float32)], axis=1).T
        near_out, far_rows, all_meta, shared_out = gather_rows(tok_rows, meta, w_gate, w_up, w_down, sh_gate, sh_up, sh_down, ep_size, slot_cap)
        return reduce_home(near_out, far_rows, all_meta, shared_out, w_gate, w_up, w_down)

    tok_spec = P(('dp', 'ep'), None)
    slot_spec = P('ep', None, None)
    return jax.shard_map(local_block, mesh=mesh,
                         in_specs=(tok_spec, P(None, None), tok_spec, tok_spec, slot_spec, slot_spec, slot_spec,
                                   P(None, None), P(None, None), P(None, None)),
                         out_specs=tok_spec, check_vma=False)
```
